32 devices in a mesh: dp: 4 (over y, z), tp: 8 (over x, core).
Axes of the slice: x: 4, y: 2, z: 2, core: 2. Of those that a mesh axis runs over, the one named last changes fastest.
The devices are a block of a 4x4x8 slice.
Arguments:
- token_ids: int32 [128, 128], P('dp'), parts along dimension 0
- emb_table: bfloat16 [16384, 1024], P('tp')
- gain_vec: bfloat16 [1024], replicated
- w_qkv: bfloat16 [1024, 11264], P(None, 'tp')
- grad_u: bfloat16 [128, 128, 11264], P('dp', None, 'tp'), parts along dimension 0
- grad_res: bfloat16 [128, 128, 1024], P('dp', 'tp'), parts along dimension 0
Outputs:
- output 1: bfloat16 [128, 128, 11264], P('dp', None, 'tp'), parts along dimension 0
- output 2: bfloat16 [128, 128, 1024], P('dp', 'tp'), parts along dimension 0
- output 3: float32 [65536, 1024], P(('dp', 'tp')), parts along dimension 0
- output 4: float32 [1024, 45056], P(None, ('dp', 'tp')), parts along dimension 1
- output 5: float32 [4096], P('dp'), parts along dimension 0
There are 4 independent parts. The reference program is written for one: setup_inputs(seed, part) draws one part's arguments, and reference() takes and returns one part's arrays. A program takes and returns all parts, laid end to end along the dimension named above; an argument that names none is the same for every part.
All inputs are finite; a program needn't handle non-finite values.
Results may differ from the reference program's by a relative error of at most 0.00497064.
Values are sent between devices in bfloat16 or wider.
A program may use at most 768 MiB of HBM per device.

```python
import jax
import jax.numpy as jnp
from jax import lax

NUM_MICRO = 32
SEQ_LEN = 128
VOCAB_ROWS = 16384
MODEL_DIM = 1024
QKV_COLS = 11264
GROUP_SIZE = 8
COLS_DEV = QKV_COLS // GROUP_SIZE
NORM_EPS = 1e-6


def setup_inputs(seed: int = 0, part: int = 0) -> dict:
    root_key = jax.random.key(seed)
    own_keys = jax.random.split(jax.random.fold_in(root_key, part), 6)
    shared_keys = jax.random.split(root_key, 3)
    spacing = VOCAB_ROWS // 64
    base_ids = jax.random.randint(own_keys[0], (NUM_MICRO, SEQ_LEN), 0, VOCAB_ROWS)
    hot_slot = jax.random.randint(own_keys[1], (NUM_MICRO, SEQ_LEN), 0, 64)
    hot_shift = jax.random.randint(own_keys[2], (), 0, spacing)
    use_hot = jax.random.randint(own_keys[3], (NUM_MICRO, SEQ_LEN), 0, 2)
    token_ids = jnp.where(use_hot == 1, hot_slot * spacing + hot_shift, base_ids)
    token_ids = token_ids.at[0, 0].set(0).at[0, 1].set(VOCAB_ROWS - 1).astype(jnp.int32)
    emb_table = jax.random.normal(shared_keys[0], (VOCAB_ROWS, MODEL_DIM), jnp.float32).astype(jnp.bfloat16)
    gain_vec = (0.5 + jax.random.uniform(shared_keys[1], (MODEL_DIM,), jnp.float32)).astype(jnp.bfloat16)
    w_qkv = (jax.random.normal(shared_keys[2], (MODEL_DIM, QKV_COLS), jnp.float32) * MODEL_DIM ** -0.5).astype(jnp.bfloat16)
    grad_u = (jax.random.normal(own_keys[4], (NUM_MICRO, SEQ_LEN, QKV_COLS), jnp.float32) * (MODEL_DIM / QKV_COLS) ** 0.5).astype(jnp.bfloat16)
    grad_res = jax.random.normal(own_keys[5], (NUM_MICRO, SEQ_LEN, MODEL_DIM), jnp.float32).astype(jnp.bfloat16)
    return {'token_ids': token_ids, 'emb_table': emb_table, 'gain_vec': gain_vec, 'w_qkv': w_qkv, 'grad_u': grad_u, 'grad_res': grad_res}


def reference(token_ids, emb_table, gain_vec, w_qkv, grad_u, grad_res):
    gain_f = gain_vec.astype(jnp.float32)

    def micro_step(acc_state, inputs):
        grad_table, grad_w, grad_gain = acc_state
        tok_ids, du_m, dres_m = inputs
        tokens = jnp.take(emb_table, tok_ids, axis=0)
        tok_f = tokens.astype(jnp.float32)
        inv_rms = lax.rsqrt(jnp.mean(tok_f * tok_f, axis=-1, keepdims=True) + NORM_EPS)
        n_hat = tok_f * inv_rms
        normed = (n_hat * gain_f).astype(jnp.bfloat16)
        u_m = jnp.dot(normed, w_qkv, preferred_element_type=jnp.float32).astype(jnp.bfloat16)

        def group_term(dn_acc, group_idx):
            du_r = lax.dynamic_slice_in_dim(du_m, group_idx * COLS_DEV, COLS_DEV, axis=1)
            w_r = lax.dynamic_slice_in_dim(w_qkv, group_idx * COLS_DEV, COLS_DEV, axis=1)
            part_dn = jnp.dot(du_r, w_r.T, preferred_element_type=jnp.float32).astype(jnp.bfloat16)
            return dn_acc + part_dn.astype(jnp.float32), None

        d_norm, _ = lax.scan(group_term, jnp.zeros((SEQ_LEN, MODEL_DIM), jnp.float32), jnp.arange(GROUP_SIZE))
        gain_dn = gain_f * d_norm
        centre = jnp.mean(n_hat * gain_dn, axis=-1, keepdims=True)
        d_x = (dres_m.astype(jnp.float32) + inv_rms * (gain_dn - n_hat * centre)).astype(jnp.bfloat16)
        grad_table = grad_table + jax.ops.segment_sum(d_x.astype(jnp.float32), tok_ids, num_segments=VOCAB_ROWS)
        grad_w = grad_w + jnp.dot(normed.T, du_m, preferred_element_type=jnp.float32)
        grad_gain = grad_gain + jnp.sum(d_norm * n_hat, axis=0)
        return (grad_table, grad_w, grad_gain), (u_m, tokens)

    init_state = (jnp.zeros((VOCAB_ROWS, MODEL_DIM), jnp.float32), jnp.zeros((MODEL_DIM, QKV_COLS), jnp.float32), jnp.zeros((MODEL_DIM,), jnp.float32))
    (grad_table, grad_w, grad_gain), (u_proj, x_resid) = lax.scan(micro_step, init_state, (token_ids, grad_u, grad_res))
    return u_proj, x_resid, grad_table, grad_w, grad_gain
```

```python
import functools
import jax
import jax.numpy as jnp
from jax import lax
from jax.experimental import pallas as pl
from jax.experimental.pallas import tpu as pltpu
from jax.sharding import PartitionSpec as P

NORM_EPS = 1e-6
LANES = 128
F32 = jnp.float32
BF16 = jnp.bfloat16
VMEM_MAX = 60 * 1024 * 1024


def _capacity(mean, slack):
    return -(-(mean * slack) // 128) * 128 // 8


def slow_step(token_ids, table_loc, gain_vec, w_loc, du_loc, dres_loc, group_size):
    seq_len = token_ids.shape[1]
    rows_loc, model_dim = table_loc.shape
    seq_loc = seq_len // group_size
    cols_loc = w_loc.shape[1]
    dev_idx = lax.axis_index('tp')
    row_start = dev_idx * rows_loc
    tok_start = dev_idx * seq_loc
    gain_f = gain_vec.astype(F32)

    def micro_step(acc_state, inputs):
        grad_table, grad_w, grad_gain = acc_state
        tok_ids, du_m, dres_m = inputs
        local_ids = tok_ids - row_start
        in_block = (local_ids >= 0) & (local_ids < rows_loc)
        safe_ids = jnp.where(in_block, local_ids, 0)
        looked = jnp.take(table_loc, safe_ids, axis=0)
        partial_x = jnp.where(in_block[:, None], looked, jnp.zeros_like(looked))
        tokens = lax.psum(partial_x, 'tp')
        tok_f = tokens.astype(F32)
        inv_rms = lax.rsqrt(jnp.mean(tok_f * tok_f, axis=-1, keepdims=True) + NORM_EPS)
        n_hat = tok_f * inv_rms
        normed = (n_hat * gain_f).astype(BF16)
        u_m = jnp.dot(normed, w_loc, preferred_element_type=F32).astype(BF16)
        x_own = lax.dynamic_slice_in_dim(tokens, tok_start, seq_loc, axis=0)
        dn_part = lax.dot_general(du_m, w_loc, (((1,), (1,)), ((), ())), preferred_element_type=F32).astype(BF16)
        dn_recv = lax.all_to_all(dn_part.reshape(group_size, seq_loc, model_dim), 'tp', 0, 0, tiled=True)
        d_norm = jnp.sum(dn_recv, axis=0, dtype=F32)
        hat_own = lax.dynamic_slice_in_dim(n_hat, tok_start, seq_loc, axis=0)
        inv_own = lax.dynamic_slice_in_dim(inv_rms, tok_start, seq_loc, axis=0)
        gain_dn = gain_f * d_norm
        centre = jnp.mean(hat_own * gain_dn, axis=-1, keepdims=True)
        d_x = (dres_m.astype(F32) + inv_own * (gain_dn - hat_own * centre)).astype(BF16)
        grad_gain = grad_gain + jnp.sum(d_norm * hat_own, axis=0)
        grad_w = grad_w + lax.dot_general(normed, du_m, (((0,), (0,)), ((), ())), preferred_element_type=F32)
        dx_all = lax.all_gather(d_x, 'tp', axis=0, tiled=True)
        contrib = jnp.where(in_block[:, None], dx_all.astype(F32), 0.0)
        grad_table = grad_table + jax.ops.segment_sum(contrib, safe_ids, num_segments=rows_loc)
        return (grad_table, grad_w, grad_gain), (u_m, x_own)

    init_state = (jnp.zeros((rows_loc, model_dim), F32), jnp.zeros((model_dim, cols_loc), F32), jnp.zeros((model_dim,), F32))
    (grad_table, grad_w, grad_gain), (u_proj, x_resid) = lax.scan(micro_step, init_state, (token_ids, du_loc, dres_loc))
    grad_gain = lax.psum(grad_gain, 'tp')
    return u_proj, x_resid, grad_table, grad_w, grad_gain


def index_tables(token_ids, rows_loc, group_size, cap, cap2):
    n_micro, seq_len = token_ids.shape
    seq_loc = seq_len // group_size
    per = n_micro * seq_loc
    me = lax.axis_index('tp')
    ids_h = token_ids.reshape(n_micro, group_size, seq_loc).transpose(1, 0, 2).reshape(group_size, per)
    owner = ids_h // rows_loc
    oh = owner[None] == jnp.arange(group_size, dtype=jnp.int32)[:, None, None]
    tri = (jnp.arange(per)[:, None] < jnp.arange(per)[None, :]).astype(BF16)
    ranks = jnp.dot(oh.reshape(group_size * group_size, per).astype(BF16), tri, preferred_element_type=F32)
    ranks = ranks.reshape(group_size, group_size, per).astype(jnp.int32)
    rk = jnp.sum(jnp.where(oh, ranks, 0), axis=0)
    cnt = jnp.sum(oh.astype(jnp.int32), axis=2)
    before = jnp.arange(group_size)[:, None] < jnp.arange(group_size)[None, :]
    base = jnp.sum(jnp.where(before[None], cnt[:, :, None], 0), axis=1)
    total = jnp.sum(cnt, axis=1)
    ok = (jnp.max(total) <= cap) & (jnp.max(cnt) <= cap2)
    grank = rk + jnp.sum(jnp.where(oh, base[:, :, None], 0), axis=0)
    gidx = owner * cap + jnp.minimum(grank, cap - 1)
    mine = jnp.where(owner == me, grank, -1).reshape(1, -1)
    row = (ids_h - me * rows_loc).reshape(1, -1)
    packid = jnp.sum(jnp.where(mine == jnp.arange(cap, dtype=jnp.int32)[:, None], row, 0), axis=1)
    slot2 = lax.dynamic_slice_in_dim(owner * cap2 + rk, me, 1, axis=0)
    inv2 = jnp.sum(jnp.where(slot2 == jnp.arange(group_size * cap2, dtype=jnp.int32)[:, None],
                             jnp.arange(per, dtype=jnp.int32)[None, :], 0), axis=1)
    base_me = lax.dynamic_slice_in_dim(base, me, 1, axis=0)[0]
    cnt_me = lax.dynamic_slice_in_dim(cnt, me, 1, axis=0)[0]
    return ok, gidx.reshape(-1), packid, inv2, base_me, cnt_me


def to_rows(dst, base, xf):
    r = xf.shape[0]
    for k in range(xf.shape[1] // LANES):
        dst[pl.ds(base * 8 + k, r, stride=8), :] = xf[:, k * LANES:(k + 1) * LANES]


def from_rows(src, base, r):
    return jnp.concatenate([src[pl.ds(base * 8 + k, r, stride=8), :] for k in range(8)], axis=1)


def gather_rows(dst, src, idx_ref, idx0, count, unroll=16):
    def body(i, c):
        for j in range(unroll):
            r = i * unroll + j
            s = pl.multiple_of(idx_ref[idx0 + r] * 8, 8)
            d = pl.multiple_of(r * 8, 8)
            dst[pl.ds(d, 8), :] = src[pl.ds(s, 8), :]
        return c
    lax.fori_loop(0, count // unroll, body, 0)


def norm_call(p_all, gidx, gain, cap, n_micro, group_size, seq_loc):
    n_rows, dim = p_all.shape
    per = n_micro * seq_loc
    sub = 64

    def kernel(gidx_ref, me_ref, p_ref, g_ref, n_ref, x_ref, land, rows, stage, sems):
        h = pl.program_id(0)

        @pl.when(h == 0)
        def _():
            def copy(o):
                return pltpu.make_async_copy(p_ref.at[pl.ds(o * cap, cap), :], land.at[o % 2], sems.at[o % 2])
            copy(0).start()
            for o in range(group_size):
                if o + 1 < group_size:
                    copy(o + 1).start()
                copy(o).wait()

                def body(c, carry):
                    off = pl.multiple_of(c * sub, sub)
                    to_rows(rows, o * cap + off, land[o % 2, pl.ds(off, sub), :].astype(F32))
                    return carry
                lax.fori_loop(0, cap // sub, body, 0)

        gather_rows(stage, rows, gidx_ref, h * per, per)
        gf = g_ref[...].astype(F32)
        for c in range(per // sub):
            xf = from_rows(stage, c * sub, sub)
            rs = lax.rsqrt(jnp.mean(xf * xf, axis=-1, keepdims=True) + NORM_EPS)
            nb = ((xf * rs) * gf).astype(BF16)
            m0 = c * sub // seq_loc
            ms = sub // seq_loc
            n_ref[pl.ds(m0, ms), 0, :, :] = nb.reshape(ms, seq_loc, dim)

            @pl.when(h == me_ref[0])
            def _():
                x_ref[pl.ds(m0, ms), :, :] = xf.astype(BF16).reshape(ms, seq_loc, dim)

    me = lax.axis_index('tp').astype(jnp.int32).reshape(1)
    return pl.pallas_call(
        kernel,
        grid_spec=pltpu.PrefetchScalarGridSpec(
            num_scalar_prefetch=2, grid=(group_size,),
            in_specs=[pl.BlockSpec(memory_space=pl.ANY), pl.BlockSpec((1, dim), lambda h, *_: (0, 0))],
            out_specs=[pl.BlockSpec((n_micro, 1, seq_loc, dim), lambda h, *_: (0, h, 0, 0)),
                       pl.BlockSpec((n_micro, seq_loc, dim), lambda h, *_: (0, 0, 0))],
            scratch_shapes=[pltpu.VMEM((2, cap, dim), BF16), pltpu.VMEM((n_rows * 8, LANES), F32),
                            pltpu.VMEM((per * 8, LANES), F32), pltpu.SemaphoreType.DMA((2,))]),
        out_shape=[jax.ShapeDtypeStruct((n_micro, group_size, seq_loc, dim), BF16),
                   jax.ShapeDtypeStruct((n_micro, seq_loc, dim), BF16)],
        compiler_params=pltpu.CompilerParams(dimension_semantics=("arbitrary",), vmem_limit_bytes=VMEM_MAX),
        cost_estimate=pl.CostEstimate(flops=12_000_000_000, bytes_accessed=18_000_000, transcendentals=0),
        name="norm_rows",
    )(gidx, me, p_all, gain.reshape(1, dim))


def dn_part_call(du4, w_loc):
    n_micro, group_size, seq_loc, cols = du4.shape
    dim = w_loc.shape[0]
    per = n_micro * seq_loc

    def kernel(du_ref, w_ref, o_ref):
        d = du_ref[...].reshape(per, cols)
        for c in range(0, dim, 256):
            o_ref[0, :, c:c + 256] = lax.dot_general(
                d, w_ref[c:c + 256, :], (((1,), (1,)), ((), ())), preferred_element_type=F32).astype(BF16)

    return pl.pallas_call(
        kernel, grid=(group_size,),
        in_specs=[pl.BlockSpec((n_micro, 1, seq_loc, cols), lambda h: (0, h, 0, 0)),
                  pl.BlockSpec((dim, cols), lambda h: (0, 0))],
        out_specs=pl.BlockSpec((1, per, dim), lambda h: (h, 0, 0)),
        out_shape=jax.ShapeDtypeStruct((group_size, per, dim), BF16),
        compiler_params=pltpu.CompilerParams(dimension_semantics=("arbitrary",), vmem_limit_bytes=VMEM_MAX),
        cost_estimate=pl.CostEstimate(flops=12_000_000_000, bytes_accessed=24_000_000, transcendentals=0),
        name="dn_part",
    )(du4, w_loc)


def dx_call(dn_recv, x_own, dres, gain, inv2):
    group_size, per, dim = dn_recv.shape
    n_micro, seq_loc, _ = x_own.shape
    slots = inv2.shape[0]
    sub = 64
    ms = sub // seq_loc
    steps = per // sub

    def kernel(inv_ref, dn_ref, x_ref, r_ref, g_ref, o_ref, dg_ref, rows, stage):
        c = pl.program_id(0)
        dn = dn_ref[0].astype(F32)
        for s in range(1, group_size):
            dn = dn + dn_ref[s].astype(F32)
        xf = x_ref[...].reshape(sub, dim).astype(F32)
        gf = g_ref[...].astype(F32)
        rs = lax.rsqrt(jnp.mean(xf * xf, axis=-1, keepdims=True) + NORM_EPS)
        nh = xf * rs
        gdn = gf * dn
        centre = jnp.mean(nh * gdn, axis=-1, keepdims=True)
        dx = (r_ref[...].reshape(sub, dim).astype(F32) + rs * (gdn - nh * centre)).astype(BF16)
        to_rows(rows, c * sub, dx.astype(F32))
        part = jnp.sum(dn * nh, axis=0, keepdims=True)

        @pl.when(c == 0)
        def _():
            dg_ref[...] = part

        @pl.when(c > 0)
        def _():
            dg_ref[...] += part

        @pl.when(c == steps - 1)
        def _():
            gather_rows(stage, rows, inv_ref, 0, slots)

            def body(i, carry):
                off = pl.multiple_of(i * sub, sub)
                o_ref[pl.ds(off, sub), :] = from_rows(stage, off, sub).astype(BF16)
                return carry
            lax.fori_loop(0, slots // sub, body, 0)

    return pl.pallas_call(
        kernel,
        grid_spec=pltpu.PrefetchScalarGridSpec(
            num_scalar_prefetch=1, grid=(steps,),
            in_specs=[pl.BlockSpec((group_size, sub, dim), lambda c, *_: (0, c, 0)),
                      pl.BlockSpec((ms, seq_loc, dim), lambda c, *_: (c, 0, 0)),
                      pl.BlockSpec((ms, seq_loc, dim), lambda c, *_: (c, 0, 0)),
                      pl.BlockSpec((1, dim), lambda c, *_: (0, 0))],
            out_specs=[pl.BlockSpec((slots, dim), lambda c, *_: (0, 0)),
                       pl.BlockSpec((1, dim), lambda c, *_: (0, 0))],
            scratch_shapes=[pltpu.VMEM((per * 8, LANES), F32), pltpu.VMEM((slots * 8, LANES), F32)]),
        out_shape=[jax.ShapeDtypeStruct((slots, dim), BF16), jax.ShapeDtypeStruct((1, dim), F32)],
        compiler_params=pltpu.CompilerParams(dimension_semantics=("arbitrary",), vmem_limit_bytes=VMEM_MAX),
        cost_estimate=pl.CostEstimate(flops=2_000_000_000, bytes_accessed=14_000_000, transcendentals=0),
        name="dx_rows",
    )(inv2, dn_recv, x_own, dres, gain.reshape(1, dim))


def table_grad_call(recv, packid, base_me, cnt_me, rows_loc, cap2):
    slots, dim = recv.shape
    group_size = slots // cap2
    sub = 64
    steps = 8
    blk = rows_loc // steps

    def kernel(id_ref, base_ref, cnt_ref, r_ref, o_ref, rows, acc):
        c = pl.program_id(0)

        @pl.when(c == 0)
        def _():
            def zero(i, carry):
                acc[pl.ds(pl.multiple_of(i * 512, 512), 512), :] = jnp.zeros((512, LANES), F32)
                return carry
            lax.fori_loop(0, rows_loc * 8 // 512, zero, 0)

            def conv(i, carry):
                off = pl.multiple_of(i * sub, sub)
                to_rows(rows, off, r_ref[pl.ds(off, sub), :].astype(F32))
                return carry
            lax.fori_loop(0, slots // sub, conv, 0)
            for h in range(group_size):
                b = base_ref[h]

                def add(r, carry):
                    t = pl.multiple_of(id_ref[b + r] * 8, 8)
                    s = pl.multiple_of((h * cap2 + r) * 8, 8)
                    acc[pl.ds(t, 8), :] += rows[pl.ds(s, 8), :]
                    return carry
                lax.fori_loop(0, cnt_ref[h], add, 0)

        for i in range(blk // sub):
            o_ref[i * sub:(i + 1) * sub, :] = from_rows(acc, c * blk + i * sub, sub)

    return pl.pallas_call(
        kernel,
        grid_spec=pltpu.PrefetchScalarGridSpec(
            num_scalar_prefetch=3, grid=(steps,),
            in_specs=[pl.BlockSpec((slots, dim), lambda c, *_: (0, 0))],
            out_specs=pl.BlockSpec((blk, dim), lambda c, *_: (c, 0)),
            scratch_shapes=[pltpu.VMEM((slots * 8, LANES), F32), pltpu.VMEM((rows_loc * 8, LANES), F32)]),
        out_shape=jax.ShapeDtypeStruct((rows_loc, dim), F32),
        compiler_params=pltpu.CompilerParams(dimension_semantics=("arbitrary",), vmem_limit_bytes=VMEM_MAX),
        cost_estimate=pl.CostEstimate(flops=2_000_000_000, bytes_accessed=12_000_000, transcendentals=0),
        name="table_grad",
    )(packid, base_me, cnt_me, recv)


def fast_step(tables, table_loc, gain_vec, w_loc, du_loc, dres_loc, group_size, cap, cap2):
    gidx, packid, inv2, base_me, cnt_me = tables
    n_micro, seq_len, cols = du_loc.shape
    seq_loc = seq_len // group_size
    rows_loc, dim = table_loc.shape
    du4 = du_loc.reshape(n_micro, group_size, seq_loc, cols)
    mine = jnp.take(table_loc, packid, axis=0)
    p_all = lax.all_gather(mine, 'tp', axis=0, tiled=True)
    dn_part = dn_part_call(du4, w_loc)
    dn_recv = lax.all_to_all(dn_part, 'tp', 0, 0, tiled=True)
    normed, x_own = norm_call(p_all, gidx, gain_vec, cap, n_micro, group_size, seq_loc)
    nt = normed.reshape(n_micro * seq_len, dim)
    u = jnp.dot(nt, w_loc, preferred_element_type=F32).astype(BF16)
    grad_w = lax.dot_general(nt, du_loc.reshape(n_micro * seq_len, cols), (((0,), (0,)), ((), ())), preferred_element_type=F32)
    dx_pack, dg = dx_call(dn_recv, x_own, dres_loc, gain_vec, inv2)
    recv = lax.all_to_all(dx_pack.reshape(group_size, cap2, dim), 'tp', 0, 0, tiled=True)
    grad_table = table_grad_call(recv.reshape(group_size * cap2, dim), packid, base_me, cnt_me, rows_loc, cap2)
    grad_gain = lax.psum(dg.reshape(dim), 'tp')
    return u.reshape(n_micro, seq_len, cols), x_own, grad_table, grad_w, grad_gain


def solution(mesh):
    group_size = mesh.shape['tp']

    def local_step(token_ids, table_loc, gain_vec, w_loc, du_loc, dres_loc):
        rows_loc = table_loc.shape[0]
        tokens = token_ids.shape[0] * token_ids.shape[1]
        cap = tokens // group_size * 5 // 4
        cap2 = tokens // group_size // group_size * 3 // 2
        ok, *tables = index_tables(token_ids, rows_loc, group_size, cap, cap2)
        return lax.cond(
            ok,
            lambda t, i, *a: fast_step(t, *a, group_size, cap, cap2),
            lambda t, i, *a: slow_step(i, *a, group_size),
            tuple(tables), token_ids, table_loc, gain_vec, w_loc, du_loc, dres_loc)

    return jax.shard_map(local_step, mesh=mesh,
                         in_specs=(P('dp', None), P('tp', None), P(None), P(None, 'tp'), P('dp', None, 'tp'), P('dp', 'tp', None)),
                         out_specs=(P('dp', None, 'tp'), P('dp', 'tp', None), P(('dp', 'tp'), None), P(None, ('dp', 'tp')), P('dp')),
                         check_vma=False)
```

```python
import functools
import jax
import jax.numpy as jnp
from jax import lax
from jax.experimental import pallas as pl
from jax.experimental.pallas import tpu as pltpu
from jax.sharding import PartitionSpec as P

NORM_EPS = 1e-6
LANES = 128
F32 = jnp.float32
BF16 = jnp.bfloat16
VMEM_MAX = 60 * 1024 * 1024


def _capacity(mean, slack):
    return -(-(mean * slack) // 128) * 128 // 8


def slow_step(token_ids, table_loc, gain_vec, w_loc, du_loc, dres_loc, group_size):
    seq_len = token_ids.shape[1]
    rows_loc, model_dim = table_loc.shape
    seq_loc = seq_len // group_size
    cols_loc = w_loc.shape[1]
    dev_idx = lax.axis_index('tp')
    row_start = dev_idx * rows_loc
    tok_start = dev_idx * seq_loc
    gain_f = gain_vec.astype(F32)

    def micro_step(acc_state, inputs):
        grad_table, grad_w, grad_gain = acc_state
        tok_ids, du_m, dres_m = inputs
        local_ids = tok_ids - row_start
        in_block = (local_ids >= 0) & (local_ids < rows_loc)
        safe_ids = jnp.where(in_block, local_ids, 0)
        looked = jnp.take(table_loc, safe_ids, axis=0)
        partial_x = jnp.where(in_block[:, None], looked, jnp.zeros_like(looked))
        spread = lax.all_to_all(partial_x.reshape(group_size, seq_loc, model_dim), 'tp', 0, 0, tiled=True)
        mine = jnp.sum(spread, axis=0, dtype=F32).astype(BF16)
        tokens = lax.all_gather(mine, 'tp', axis=0, tiled=True)
        tok_f = tokens.astype(F32)
        inv_rms = lax.rsqrt(jnp.mean(tok_f * tok_f, axis=-1, keepdims=True) + NORM_EPS)
        n_hat = tok_f * inv_rms
        normed = (n_hat * gain_f).astype(BF16)
        u_m = jnp.dot(normed, w_loc, preferred_element_type=F32).astype(BF16)
        x_own = lax.dynamic_slice_in_dim(tokens, tok_start, seq_loc, axis=0)
        dn_part = lax.dot_general(du_m, w_loc, (((1,), (1,)), ((), ())), preferred_element_type=F32).astype(BF16)
        dn_recv = lax.all_to_all(dn_part.reshape(group_size, seq_loc, model_dim), 'tp', 0, 0, tiled=True)
        d_norm = jnp.sum(dn_recv, axis=0, dtype=F32)
        hat_own = lax.dynamic_slice_in_dim(n_hat, tok_start, seq_loc, axis=0)
        inv_own = lax.dynamic_slice_in_dim(inv_rms, tok_start, seq_loc, axis=0)
        gain_dn = gain_f * d_norm
        centre = jnp.mean(hat_own * gain_dn, axis=-1, keepdims=True)
        d_x = (dres_m.astype(F32) + inv_own * (gain_dn - hat_own * centre)).astype(BF16)
        grad_gain = grad_gain + jnp.sum(d_norm * hat_own, axis=0)
        grad_w = grad_w + lax.dot_general(normed, du_m, (((0,), (0,)), ((), ())), preferred_element_type=F32)
        dx_all = lax.all_gather(d_x, 'tp', axis=0, tiled=True)
        contrib = jnp.where(in_block[:, None], dx_all.astype(F32), 0.0)
        grad_table = grad_table + jax.ops.segment_sum(contrib, safe_ids, num_segments=rows_loc)
        return (grad_table, grad_w, grad_gain), (u_m, x_own)

    init_state = (jnp.zeros((rows_loc, model_dim), F32), jnp.zeros((model_dim, cols_loc), F32), jnp.zeros((model_dim,), F32))
    (grad_table, grad_w, grad_gain), (u_proj, x_resid) = lax.scan(micro_step, init_state, (token_ids, du_loc, dres_loc))
    grad_gain = lax.psum(grad_gain, 'tp')
    return u_proj, x_resid, grad_table, grad_w, grad_gain


def pack_call(token_ids, table_loc, group_size, cap, cap2):
    n_micro, seq_len = token_ids.shape
    seq_loc = seq_len // group_size
    per = n_micro * seq_loc
    rows_loc, dim = table_loc.shape
    slots = group_size * cap2
    pairs = group_size * group_size
    sub = 64
    ids_h = token_ids.reshape(n_micro, group_size, seq_loc).transpose(1, 0, 2).reshape(group_size, per)

    def kernel(ids_ref, e_ref, gidx_ref, pid_ref, inv_ref, stat_ref, p_ref, rows, stage, pid_s, sem):
        me = lax.axis_index('tp')
        ids = ids_ref[...]
        owner = ids // rows_loc
        oh = jnp.concatenate([(owner == o).astype(F32) for o in range(group_size)], axis=0)
        ohb = oh.astype(BF16)
        tri = (lax.broadcasted_iota(jnp.int32, (per, per), 0) < lax.broadcasted_iota(jnp.int32, (per, per), 1)).astype(F32).astype(BF16)
        rank = jnp.dot(ohb, tri, preferred_element_type=F32)
        nt = (((1,), (1,)), ((), ()))
        cnt_row = lax.dot_general(jnp.ones((8, per), BF16), ohb, nt, preferred_element_type=F32)[0:1]
        cnt_col = jnp.sum(oh, axis=1, keepdims=True)
        ra = lax.broadcasted_iota(jnp.int32, (pairs, pairs), 0)
        rb = lax.broadcasted_iota(jnp.int32, (pairs, pairs), 1)
        same = ra // group_size == rb // group_size
        base_col = jnp.sum(jnp.where(same & (rb < ra), cnt_row, 0.0), axis=1, keepdims=True)
        base_row = jnp.sum(jnp.where(same & (ra < rb), cnt_col, 0.0), axis=0, keepdims=True)
        tot_row = jnp.sum(jnp.where(same, cnt_col, 0.0), axis=0, keepdims=True)
        worst = jnp.concatenate([jnp.max(tot_row, axis=1, keepdims=True), jnp.max(cnt_row, axis=1, keepdims=True)], axis=0)

        def fold(v):
            s = v[0:group_size]
            for o in range(1, group_size):
                s = s + v[o * group_size:(o + 1) * group_size]
            return s.astype(jnp.int32)

        rk = fold(oh * rank)
        grank = fold(oh * (rank + base_col))
        gidx_ref[...] = owner * cap + jnp.minimum(grank, cap - 1)
        stat_ref[0:1, :] = cnt_row.astype(jnp.int32)
        stat_ref[1:2, :] = base_row.astype(jnp.int32)
        stat_ref[2:4, :] = jnp.broadcast_to(worst, (2, pairs)).astype(jnp.int32)
        stat_ref[4:8, :] = jnp.zeros((4, pairs), jnp.int32)

        def place(slot, value, n):
            hot = (slot == lax.broadcasted_iota(jnp.int32, (n, per), 0)).astype(F32).astype(BF16)
            parts = jnp.concatenate([value // 64, value % 64] + [jnp.zeros_like(value)] * 6, axis=0).astype(F32).astype(BF16)
            return lax.dot_general(parts, hot, nt, preferred_element_type=F32)

        mine = jnp.where(owner == me, grank, -1)
        local = jnp.clip(ids - me * rows_loc, 0, rows_loc - 1)
        acc = jnp.zeros((8, cap), F32)
        for h in range(group_size):
            acc = acc + place(mine[h:h + 1], local[h:h + 1], cap)
        pid = (acc[0:1] * 64.0 + acc[1:2]).astype(jnp.int32)
        pid_ref[...] = pid
        own = lax.broadcasted_iota(jnp.int32, (group_size, 1), 0) == me
        slot2 = jnp.sum(jnp.where(own, owner * cap2 + rk, 0), axis=0, keepdims=True)
        put = place(slot2, lax.broadcasted_iota(jnp.int32, (1, per), 1), slots)
        inv_ref[...] = (put[0:1] * 64.0 + put[1:2]).astype(jnp.int32)
        cp = pltpu.make_async_copy(pid_ref, pid_s, sem)
        cp.start()

        def conv(i, carry):
            off = pl.multiple_of(i * sub, sub)
            to_rows(rows, off, e_ref[pl.ds(off, sub), :].astype(F32))
            return carry
        lax.fori_loop(0, rows_loc // sub, conv, 0)
        cp.wait()
        gather_rows(stage, rows, lambda r: pid_s[0, r], cap)

        def back(i, carry):
            off = pl.multiple_of(i * sub, sub)
            p_ref[pl.ds(off, sub), :] = from_rows(stage, off, sub).astype(BF16)
            return carry
        lax.fori_loop(0, cap // sub, back, 0)

    vspec = pl.BlockSpec(memory_space=pltpu.VMEM)
    return pl.pallas_call(
        kernel,
        in_specs=[vspec, vspec],
        out_specs=[vspec] * 5,
        out_shape=[jax.ShapeDtypeStruct((group_size, per), jnp.int32),
                   jax.ShapeDtypeStruct((1, cap), jnp.int32),
                   jax.ShapeDtypeStruct((1, slots), jnp.int32),
                   jax.ShapeDtypeStruct((8, pairs), jnp.int32),
                   jax.ShapeDtypeStruct((cap, dim), BF16)],
        scratch_shapes=[pltpu.VMEM((rows_loc, 8, LANES), F32), pltpu.VMEM((cap, 8, LANES), F32),
                        pltpu.SMEM((1, cap), jnp.int32), pltpu.SemaphoreType.DMA(())],
        compiler_params=pltpu.CompilerParams(vmem_limit_bytes=VMEM_MAX),
        name="pack_rows",
    )(ids_h, table_loc)


def flat(ref):
    return ref.reshape(ref.shape[0] * 8, LANES)


def to_rows(dst, base, xf):
    r = xf.shape[0]
    for k in range(8):
        flat(dst)[pl.ds(base * 8 + k, r, stride=8), :] = xf[:, k * LANES:(k + 1) * LANES]


def from_rows(src, base, r):
    return jnp.concatenate([flat(src)[pl.ds(base * 8 + k, r, stride=8), :] for k in range(8)], axis=1)


def gather_rows(dst, src, index, count, unroll=16):
    def body(i, c):
        for j in range(unroll):
            r = i * unroll + j
            dst[r] = src[index(r)]
        return c
    lax.fori_loop(0, count // unroll, body, 0)


def group_call(p_own, gidx, inv2, gain, w_loc, du4, dres, cap, cap2):
    n_micro, group_size, seq_loc, cols = du4.shape
    chips = group_size // 2
    dim = w_loc.shape[0]
    per = n_micro * seq_loc
    half = per // 2
    piece = half // 2
    hcap = cap // 2
    slots = group_size * cap2
    sub = 64
    far = chips // 2

    def kernel(gidx_ref, inv_ref, p_ref, g_ref, w_ref, du_ref, r_ref,
               pall_ref, n_ref, x_ref, pack_ref, dg_ref, dw_ref,
               rows, land, stage, nbuf, ntr, dub, part, relay_in, relay_p, relay_out,
               own_p, direct, summed, dg_all, land_sem, du_sem, n_sem, send, recv):
        me = lax.axis_index('tp')
        c = me // 2
        k = me % 2

        def dev(chip_off, core):
            return ((c + chip_off) % chips) * 2 + core

        right, left, partner = dev(1, k), dev(chips - 1, k), dev(0, 1 - k)
        barrier = pltpu.get_barrier_semaphore()
        for o in range(1, group_size):
            pl.semaphore_signal(barrier, inc=1, device_id={'tp': (me + o) % group_size}, device_id_type=pl.DeviceIdType.MESH)
        pl.semaphore_wait(barrier, group_size - 1)

        def rcopy(src, dst, s, r, to):
            return pltpu.make_async_remote_copy(src_ref=src, dst_ref=dst, send_sem=send.at[s], recv_sem=recv.at[r],
                                                device_id={'tp': to}, device_id_type=pl.DeviceIdType.MESH)

        def arrived(dst, r):
            pltpu.make_async_remote_copy(src_ref=dst, dst_ref=dst, send_sem=send.at[0], recv_sem=recv.at[r],
                                         device_id={'tp': partner}, device_id_type=pl.DeviceIdType.MESH).wait_recv()

        sent = []

        def go(cp):
            cp.start()
            sent.append(cp)

        def blk(d, off=0, n=cap):
            return pall_ref.at[pl.ds(pl.multiple_of(d * cap + off, 16), n), :]

        go(rcopy(p_ref, blk(me), 0, 0, right))
        go(rcopy(p_ref, blk(me), 1, 1, left))
        go(rcopy(p_ref, blk(me), 2, 2, partner))

        def du_copy(d, slot):
            return pltpu.make_async_copy(du_ref.at[:, d], dub.at[slot], du_sem.at[slot])

        def order(j):
            return ((c + far + j // 2) % chips) * 2 + j % 2

        du_copy(order(0), 0).start()

        def dn_body(j, carry):
            slot = j % 2

            @pl.when(j + 1 < group_size)
            def _():
                du_copy(order(j + 1), 1 - slot).start()
            du_copy(order(j), slot).wait()
            d = order(j)
            dv = dub[slot].reshape(per, cols)
            for t in range(0, dim, 256):
                part[d, :, t:t + 256] = lax.dot_general(
                    dv, w_ref[t:t + 256, :], (((1,), (1,)), ((), ())), preferred_element_type=F32).astype(BF16)
            return carry
        lax.fori_loop(0, group_size, dn_body, 0)

        du_copy(0, 0).start()

        def first_hop(kk):
            d = dev(far, kk)
            go(rcopy(part.at[d, pl.ds(0, half)], relay_in.at[0, k], 9 + kk, 9 + k, dev(chips - 1, kk)))
            go(rcopy(part.at[d, pl.ds(half, half)], relay_in.at[1, k], 11 + kk, 11 + k, dev(1, kk)))

        first_hop(0)
        dl, dr = dev(chips - 1, 1 - k), dev(1, 1 - k)
        go(rcopy(part.at[dl, pl.ds(0, half)], relay_p.at[0], 17, 17, partner))
        go(rcopy(part.at[dr, pl.ds(half, half)], relay_p.at[1], 18, 18, partner))
        go(rcopy(part.at[partner], own_p, 19, 19, partner))

        def convert(src, base, n):
            cp = pltpu.make_async_copy(src, land.at[pl.ds(0, n), :], land_sem)
            cp.start()
            cp.wait()

            def body(i, carry):
                off = pl.multiple_of(i * sub, sub)
                to_rows(rows, base + off, land[pl.ds(off, sub), :].astype(F32))
                return carry
            lax.fori_loop(0, n // sub, body, 0)

        convert(p_ref, me * cap, cap)
        arrived(blk(partner), 2)
        convert(blk(partner), partner * cap, cap)

        arrived(blk(left), 0)
        go(rcopy(blk(left, 0, hcap), blk(left, 0, hcap), 3, 3, right))
        arrived(blk(right), 1)
        go(rcopy(blk(right, hcap, hcap), blk(right, hcap, hcap), 4, 4, left))
        go(rcopy(blk(left), blk(left), 5, 5, partner))
        go(rcopy(blk(right), blk(right), 6, 6, partner))
        first_hop(1)
        for kk in range(2):
            go(rcopy(part.at[dev(chips - 1, kk), pl.ds(half, half)], direct.at[1, k], 13 + kk, 13 + k, dev(chips - 1, kk)))
            go(rcopy(part.at[dev(1, kk), pl.ds(0, half)], direct.at[0, k], 15 + kk, 15 + k, dev(1, kk)))
        convert(blk(left), left * cap, cap)
        convert(blk(right), right * cap, cap)
        pl_, pr_ = dev(chips - 1, 1 - k), dev(1, 1 - k)
        arrived(blk(pl_), 5)
        convert(blk(pl_), pl_ * cap, cap)
        arrived(blk(pr_), 6)
        convert(blk(pr_), pr_ * cap, cap)
        fk, fp = dev(far, k), dev(far, 1 - k)
        arrived(blk(fk, 0, hcap), 3)
        go(rcopy(blk(fk, 0, hcap), blk(fk, 0, hcap), 7, 7, partner))
        arrived(blk(fk, hcap, hcap), 4)
        go(rcopy(blk(fk, hcap, hcap), blk(fk, hcap, hcap), 8, 8, partner))
        convert(blk(fk), fk * cap, cap)
        arrived(blk(fp, 0, hcap), 7)
        arrived(blk(fp, hcap, hcap), 8)
        convert(blk(fp), fp * cap, cap)

        relays = [[rcopy(relay_out.at[s, pl.ds(q * piece, piece)], summed.at[s, pl.ds(q * piece, piece)],
                         20 + 2 * s + q, 20 + 2 * s + q, left if s == 0 else right) for q in range(2)] for s in range(2)]

        def relay():
            for s in range(2):
                d = left if s == 0 else right
                arrived(relay_p.at[s], 17 + s)
                for kk in range(2):
                    arrived(relay_in.at[s, kk], 9 + 2 * s + kk)
                for q in range(2):
                    def body(i, carry):
                        o = pl.multiple_of(q * piece + i * sub, sub)
                        a = part[d, pl.ds(pl.multiple_of(s * half + o, sub), sub), :].astype(F32)
                        a = a + relay_p[s, pl.ds(o, sub), :].astype(F32)
                        a = a + relay_in[s, 0, pl.ds(o, sub), :].astype(F32)
                        a = a + relay_in[s, 1, pl.ds(o, sub), :].astype(F32)
                        relay_out[s, pl.ds(o, sub), :] = a
                        return carry
                    lax.fori_loop(0, piece // sub, body, 0)
            for q in range(2):
                for s in range(2):
                    relays[s][q].start()

        gf = g_ref[...].astype(F32)

        def n_copy(h, slot):
            return pltpu.make_async_copy(nbuf.at[slot], n_ref.at[:, h], n_sem.at[slot])

        def chunk(h, carry):
            slot = h % 2

            @pl.when(h == 2)
            def _():
                relay()

            @pl.when(h + 1 < group_size)
            def _():
                du_copy(h + 1, 1 - slot).start()
            gather_rows(stage, rows, lambda r: gidx_ref[h, r], per)

            @pl.when(h >= 2)
            def _():
                n_copy(h - 2, slot).wait()

            def norm(i, carry2):
                off = pl.multiple_of(i * sub, sub)
                ms = sub // seq_loc
                xf = from_rows(stage, off, sub)
                rs = lax.rsqrt(jnp.mean(xf * xf, axis=-1, keepdims=True) + NORM_EPS)
                nb = ((xf * rs) * gf).astype(BF16)
                nbuf[slot, pl.ds(i * ms, ms)] = nb.reshape(ms, seq_loc, dim)

                @pl.when(h == me)
                def _():
                    x_ref[pl.ds(i * ms, ms)] = xf.astype(BF16).reshape(ms, seq_loc, dim)
                return carry2
            lax.fori_loop(0, per // sub, norm, 0)
            n_copy(h, slot).start()
            ntr[...] = nbuf[slot].reshape(per, dim).T
            du_copy(h, slot).wait()
            for t in range(0, cols, 256):
                w = min(256, cols - t)
                dv = dub[slot, :, :, t:t + w].reshape(per, w)
                contrib = jnp.dot(ntr[...], dv, preferred_element_type=F32)

                @pl.when(h == 0)
                def _():
                    dw_ref[:, t:t + w] = contrib

                @pl.when(h > 0)
                def _():
                    dw_ref[:, t:t + w] += contrib
            return carry
        lax.fori_loop(0, group_size, chunk, 0)
        n_copy(group_size - 2, 0).wait()
        n_copy(group_size - 1, 1).wait()

        arrived(own_p, 19)
        for kk in range(2):
            arrived(direct.at[0, kk], 15 + kk)
            arrived(direct.at[1, kk], 13 + kk)
        for q in range(2):
            for s in range(2):
                arrived(summed.at[s, pl.ds(q * piece, piece)], 20 + 2 * s + q)

                def body(i, acc):
                    ms = sub // seq_loc
                    o = pl.multiple_of(q * piece + i * sub, sub)
                    f = pl.multiple_of(s * half + o, sub)
                    dn = summed[s, pl.ds(o, sub), :] + part[me, pl.ds(f, sub), :].astype(F32)
                    dn = dn + own_p[pl.ds(f, sub), :].astype(F32)
                    dn = dn + direct[s, 0, pl.ds(o, sub), :].astype(F32)
                    dn = dn + direct[s, 1, pl.ds(o, sub), :].astype(F32)
                    m0 = f // seq_loc
                    xf = x_ref[pl.ds(m0, ms)].reshape(sub, dim).astype(F32)
                    rs = lax.rsqrt(jnp.mean(xf * xf, axis=-1, keepdims=True) + NORM_EPS)
                    nh = xf * rs
                    gdn = gf * dn
                    centre = jnp.mean(nh * gdn, axis=-1, keepdims=True)
                    dres_f = r_ref[pl.ds(m0, ms)].reshape(sub, dim).astype(F32)
                    dx = (dres_f + rs * (gdn - nh * centre)).astype(BF16)
                    to_rows(stage, f, dx.astype(F32))
                    return acc + jnp.sum(dn * nh, axis=0, keepdims=True)
                got = lax.fori_loop(0, piece // sub, body, jnp.zeros((1, dim), F32))
                if q == 0 and s == 0:
                    dg_all[me] = got
                else:
                    dg_all[me] += got

        for o in range(1, group_size):
            go(rcopy(dg_all.at[me], dg_all.at[me], 23 + o, 23 + o, (me + o) % group_size))
        gather_rows(rows, stage, lambda r: inv_ref[0, r], slots)

        def out(i, carry):
            off = pl.multiple_of(i * sub, sub)
            pack_ref[pl.ds(off, sub), :] = from_rows(rows, off, sub).astype(BF16)
            return carry
        lax.fori_loop(0, slots // sub, out, 0)
        for o in range(1, group_size):
            arrived(dg_all.at[(me + group_size - o) % group_size], 23 + o)
        dg = dg_all[0]
        for o in range(1, group_size):
            dg = dg + dg_all[o]
        dg_ref[...] = dg
        for cp in sent:
            cp.wait_send()
        for s in range(2):
            for q in range(2):
                relays[s][q].wait_send()

    anyspec = pl.BlockSpec(memory_space=pl.ANY)
    vspec = pl.BlockSpec(memory_space=pltpu.VMEM)
    sspec = pl.BlockSpec(memory_space=pltpu.SMEM)
    return pl.pallas_call(
        kernel,
        in_specs=[sspec, sspec, anyspec, vspec, vspec, anyspec, vspec],
        out_specs=[anyspec, anyspec, vspec, vspec, vspec, vspec],
        out_shape=[jax.ShapeDtypeStruct((group_size * cap, dim), BF16),
                   jax.ShapeDtypeStruct((n_micro, group_size, seq_loc, dim), BF16),
                   jax.ShapeDtypeStruct((n_micro, seq_loc, dim), BF16),
                   jax.ShapeDtypeStruct((slots, dim), BF16),
                   jax.ShapeDtypeStruct((1, dim), F32),
                   jax.ShapeDtypeStruct((dim, cols), F32)],
        scratch_shapes=[pltpu.VMEM((group_size * cap, 8, LANES), F32),
                        pltpu.VMEM((cap, dim), BF16),
                        pltpu.VMEM((per, 8, LANES), F32),
                        pltpu.VMEM((2, n_micro, seq_loc, dim), BF16),
                        pltpu.VMEM((dim, per), BF16),
                        pltpu.VMEM((2, n_micro, seq_loc, cols), BF16),
                        pltpu.VMEM((group_size, per, dim), BF16),
                        pltpu.VMEM((2, 2, half, dim), BF16),
                        pltpu.VMEM((2, half, dim), BF16),
                        pltpu.VMEM((2, half, dim), F32),
                        pltpu.VMEM((per, dim), BF16),
                        pltpu.VMEM((2, 2, half, dim), BF16),
                        pltpu.VMEM((2, half, dim), F32),
                        pltpu.VMEM((group_size, 1, dim), F32),
                        pltpu.SemaphoreType.DMA(()),
                        pltpu.SemaphoreType.DMA((2,)),
                        pltpu.SemaphoreType.DMA((2,)),
                        pltpu.SemaphoreType.DMA((32,)),
                        pltpu.SemaphoreType.DMA((32,))],
        compiler_params=pltpu.CompilerParams(collective_id=0, has_side_effects=True, vmem_limit_bytes=66_900_000),
        name="group_rows",
    )(gidx, inv2, p_own, gain.reshape(1, dim), w_loc, du4, dres)


def table_grad_call(recv, packid, stat, rows_loc, cap2):
    slots, dim = recv.shape
    group_size = slots // cap2
    sub = 64
    steps = 8
    blk = rows_loc // steps

    def kernel(id_ref, stat_ref, r_ref, o_ref, rows, acc):
        c = pl.program_id(0)
        first = lax.axis_index('tp') * group_size

        @pl.when(c == 0)
        def _():
            def zero(i, carry):
                acc[pl.ds(i * sub, sub)] = jnp.zeros((sub, 8, LANES), F32)
                return carry
            lax.fori_loop(0, rows_loc // sub, zero, 0)

            def conv(i, carry):
                off = pl.multiple_of(i * sub, sub)
                to_rows(rows, off, r_ref[pl.ds(off, sub), :].astype(F32))
                return carry
            lax.fori_loop(0, slots // sub, conv, 0)
            for h in range(group_size):
                b = stat_ref[1, first + h]

                def add(r, carry):
                    t = id_ref[0, b + r]
                    acc[t] += rows[h * cap2 + r]
                    return carry
                lax.fori_loop(0, stat_ref[0, first + h], add, 0)

        for i in range(blk // sub):
            o_ref[i * sub:(i + 1) * sub, :] = from_rows(acc, c * blk + i * sub, sub)

    return pl.pallas_call(
        kernel,
        grid_spec=pltpu.PrefetchScalarGridSpec(
            num_scalar_prefetch=2, grid=(steps,),
            in_specs=[pl.BlockSpec((slots, dim), lambda c, *_: (0, 0))],
            out_specs=pl.BlockSpec((blk, dim), lambda c, *_: (c, 0)),
            scratch_shapes=[pltpu.VMEM((slots, 8, LANES), F32), pltpu.VMEM((rows_loc, 8, LANES), F32)]),
        out_shape=jax.ShapeDtypeStruct((rows_loc, dim), F32),
        compiler_params=pltpu.CompilerParams(dimension_semantics=("arbitrary",), vmem_limit_bytes=VMEM_MAX),
        cost_estimate=pl.CostEstimate(flops=2_000_000_000, bytes_accessed=12_000_000, transcendentals=0),
        name="table_grad",
    )(packid, stat, recv)


def fast_step(tables, table_loc, gain_vec, w_loc, du_loc, dres_loc, group_size, cap, cap2):
    gidx, packid, inv2, stat, mine = tables
    n_micro, seq_len, cols = du_loc.shape
    seq_loc = seq_len // group_size
    rows_loc, dim = table_loc.shape
    du4 = du_loc.reshape(n_micro, group_size, seq_loc, cols)
    _, normed, x_own, dx_pack, dg, grad_w = group_call(mine, gidx, inv2, gain_vec, w_loc, du4, dres_loc, cap, cap2)
    nt = normed.reshape(n_micro * seq_len, dim)
    u = jnp.dot(nt, w_loc, preferred_element_type=F32).astype(BF16)
    recv = lax.all_to_all(dx_pack.reshape(group_size, cap2, dim), 'tp', 0, 0, tiled=True)
    grad_table = table_grad_call(recv.reshape(group_size * cap2, dim), packid, stat, rows_loc, cap2)
    grad_gain = dg.reshape(dim)
    return u.reshape(n_micro, seq_len, cols), x_own, grad_table, grad_w, grad_gain


def solution(mesh):
    group_size = mesh.shape['tp']

    def local_step(token_ids, table_loc, gain_vec, w_loc, du_loc, dres_loc):
        rows_loc = table_loc.shape[0]
        tokens = token_ids.shape[0] * token_ids.shape[1]
        cap = tokens // group_size * 5 // 4
        cap2 = tokens // group_size // group_size * 3 // 2
        tables = pack_call(token_ids, table_loc, group_size, cap, cap2)
        ok = (tables[3][2, 0] <= cap) & (tables[3][3, 0] <= cap2)
        return lax.cond(
            ok,
            lambda t, i, *a: fast_step(t, *a, group_size, cap, cap2),
            lambda t, i, *a: slow_step(i, *a, group_size),
            tuple(tables), token_ids, table_loc, gain_vec, w_loc, du_loc, dres_loc)

    return jax.shard_map(local_step, mesh=mesh,
                         in_specs=(P('dp', None), P('tp', None), P(None), P(None, 'tp'), P('dp', None, 'tp'), P('dp', 'tp', None)),
                         out_specs=(P('dp', None, 'tp'), P('dp', 'tp', None), P(('dp', 'tp'), None), P(None, ('dp', 'tp')), P('dp')),
                         check_vma=False)
```

```python
import functools
import jax
import jax.numpy as jnp
from jax import lax
from jax.experimental import pallas as pl
from jax.experimental.pallas import tpu as pltpu
from jax.sharding import PartitionSpec as P

NORM_EPS = 1e-6
LANES = 128
F32 = jnp.float32
BF16 = jnp.bfloat16
VMEM_MAX = 60 * 1024 * 1024


def _capacity(mean, slack):
    return -(-(mean * slack) // 128) * 128 // 8


def slow_step(token_ids, table_loc, gain_vec, w_loc, du_loc, dres_loc, group_size):
    seq_len = token_ids.shape[1]
    rows_loc, model_dim = table_loc.shape
    seq_loc = seq_len // group_size
    cols_loc = w_loc.shape[1]
    dev_idx = lax.axis_index('tp')
    row_start = dev_idx * rows_loc
    tok_start = dev_idx * seq_loc
    gain_f = gain_vec.astype(F32)

    def micro_step(acc_state, inputs):
        grad_table, grad_w, grad_gain = acc_state
        tok_ids, du_m, dres_m = inputs
        local_ids = tok_ids - row_start
        in_block = (local_ids >= 0) & (local_ids < rows_loc)
        safe_ids = jnp.where(in_block, local_ids, 0)
        looked = jnp.take(table_loc, safe_ids, axis=0)
        partial_x = jnp.where(in_block[:, None], looked, jnp.zeros_like(looked))
        spread = lax.all_to_all(partial_x.reshape(group_size, seq_loc, model_dim), 'tp', 0, 0, tiled=True)
        mine = jnp.sum(spread, axis=0, dtype=F32).astype(BF16)
        tokens = lax.all_gather(mine, 'tp', axis=0, tiled=True)
        tok_f = tokens.astype(F32)
        inv_rms = lax.rsqrt(jnp.mean(tok_f * tok_f, axis=-1, keepdims=True) + NORM_EPS)
        n_hat = tok_f * inv_rms
        normed = (n_hat * gain_f).astype(BF16)
        u_m = jnp.dot(normed, w_loc, preferred_element_type=F32).astype(BF16)
        x_own = lax.dynamic_slice_in_dim(tokens, tok_start, seq_loc, axis=0)
        dn_part = lax.dot_general(du_m, w_loc, (((1,), (1,)), ((), ())), preferred_element_type=F32).astype(BF16)
        dn_recv = lax.all_to_all(dn_part.reshape(group_size, seq_loc, model_dim), 'tp', 0, 0, tiled=True)
        d_norm = jnp.sum(dn_recv, axis=0, dtype=F32)
        hat_own = lax.dynamic_slice_in_dim(n_hat, tok_start, seq_loc, axis=0)
        inv_own = lax.dynamic_slice_in_dim(inv_rms, tok_start, seq_loc, axis=0)
        gain_dn = gain_f * d_norm
        centre = jnp.mean(hat_own * gain_dn, axis=-1, keepdims=True)
        d_x = (dres_m.astype(F32) + inv_own * (gain_dn - hat_own * centre)).astype(BF16)
        grad_gain = grad_gain + jnp.sum(d_norm * hat_own, axis=0)
        grad_w = grad_w + lax.dot_general(normed, du_m, (((0,), (0,)), ((), ())), preferred_element_type=F32)
        dx_all = lax.all_gather(d_x, 'tp', axis=0, tiled=True)
        contrib = jnp.where(in_block[:, None], dx_all.astype(F32), 0.0)
        grad_table = grad_table + jax.ops.segment_sum(contrib, safe_ids, num_segments=rows_loc)
        return (grad_table, grad_w, grad_gain), (u_m, x_own)

    init_state = (jnp.zeros((rows_loc, model_dim), F32), jnp.zeros((model_dim, cols_loc), F32), jnp.zeros((model_dim,), F32))
    (grad_table, grad_w, grad_gain), (u_proj, x_resid) = lax.scan(micro_step, init_state, (token_ids, du_loc, dres_loc))
    grad_gain = lax.psum(grad_gain, 'tp')
    return u_proj, x_resid, grad_table, grad_w, grad_gain


def pack_call(token_ids, table_loc, group_size, cap, cap2):
    n_micro, seq_len = token_ids.shape
    seq_loc = seq_len // group_size
    per = n_micro * seq_loc
    rows_loc, dim = table_loc.shape
    slots = group_size * cap2
    pairs = group_size * group_size
    sub = 64
    ids_h = token_ids.reshape(n_micro, group_size, seq_loc).transpose(1, 0, 2).reshape(group_size, per)

    def kernel(ids_ref, e_ref, gidx_ref, pid_ref, inv_ref, stat_ref, tgt_ref, p_ref, rows, stage, pid_s, sem):
        me = lax.axis_index('tp')
        ids = ids_ref[...]
        owner = ids // rows_loc
        oh = jnp.concatenate([(owner == o).astype(F32) for o in range(group_size)], axis=0)
        ohb = oh.astype(BF16)
        tri = (lax.broadcasted_iota(jnp.int32, (per, per), 0) < lax.broadcasted_iota(jnp.int32, (per, per), 1)).astype(F32).astype(BF16)
        rank = jnp.dot(ohb, tri, preferred_element_type=F32)
        nt = (((1,), (1,)), ((), ()))
        cnt_row = lax.dot_general(jnp.ones((8, per), BF16), ohb, nt, preferred_element_type=F32)[0:1]
        cnt_col = jnp.sum(oh, axis=1, keepdims=True)
        ra = lax.broadcasted_iota(jnp.int32, (pairs, pairs), 0)
        rb = lax.broadcasted_iota(jnp.int32, (pairs, pairs), 1)
        same = ra // group_size == rb // group_size
        base_col = jnp.sum(jnp.where(same & (rb < ra), cnt_row, 0.0), axis=1, keepdims=True)
        base_row = jnp.sum(jnp.where(same & (ra < rb), cnt_col, 0.0), axis=0, keepdims=True)
        tot_row = jnp.sum(jnp.where(same, cnt_col, 0.0), axis=0, keepdims=True)
        worst = jnp.concatenate([jnp.max(tot_row, axis=1, keepdims=True), jnp.max(cnt_row, axis=1, keepdims=True)], axis=0)

        def fold(v):
            s = v[0:group_size]
            for o in range(1, group_size):
                s = s + v[o * group_size:(o + 1) * group_size]
            return s.astype(jnp.int32)

        rk = fold(oh * rank)
        grank = fold(oh * (rank + base_col))
        gidx_ref[...] = owner * cap + jnp.minimum(grank, cap - 1)
        stat_ref[0:1, :] = cnt_row.astype(jnp.int32)
        stat_ref[1:2, :] = base_row.astype(jnp.int32)
        stat_ref[2:4, :] = jnp.broadcast_to(worst, (2, pairs)).astype(jnp.int32)
        stat_ref[4:8, :] = jnp.zeros((4, pairs), jnp.int32)

        def place(slot, value, n):
            hot = (slot == lax.broadcasted_iota(jnp.int32, (n, per), 0)).astype(F32).astype(BF16)
            parts = jnp.concatenate([value // 64, value % 64] + [jnp.zeros_like(value)] * 6, axis=0).astype(F32).astype(BF16)
            return lax.dot_general(parts, hot, nt, preferred_element_type=F32)

        mine = jnp.where(owner == me, grank, -1)
        local = jnp.clip(ids - me * rows_loc, 0, rows_loc - 1)
        acc = jnp.zeros((8, cap), F32)
        for h in range(group_size):
            acc = acc + place(mine[h:h + 1], local[h:h + 1], cap)
        pid = (acc[0:1] * 64.0 + acc[1:2]).astype(jnp.int32)
        pid_ref[...] = pid
        pair = jnp.where(owner == me, rk, -1)
        for h in range(group_size):
            got = place(pair[h:h + 1], local[h:h + 1] + 1, cap2)
            row = (got[0:1] * 64.0 + got[1:2]).astype(jnp.int32)
            tgt_ref[h:h + 1, :] = jnp.where(row == 0, rows_loc, row - 1)
        own = lax.broadcasted_iota(jnp.int32, (group_size, 1), 0) == me
        slot2 = jnp.sum(jnp.where(own, owner * cap2 + rk, 0), axis=0, keepdims=True)
        put = place(slot2, lax.broadcasted_iota(jnp.int32, (1, per), 1), slots)
        inv_ref[...] = (put[0:1] * 64.0 + put[1:2]).astype(jnp.int32)
        cp = pltpu.make_async_copy(pid_ref, pid_s, sem)
        cp.start()

        def conv(i, carry):
            off = pl.multiple_of(i * sub, sub)
            to_rows(rows, off, e_ref[pl.ds(off, sub), :].astype(F32))
            return carry
        lax.fori_loop(0, rows_loc // sub, conv, 0)
        cp.wait()
        gather_rows(stage, rows, lambda r: pid_s[0, r], cap)

        def back(i, carry):
            off = pl.multiple_of(i * sub, sub)
            p_ref[pl.ds(off, sub), :] = from_rows(stage, off, sub).astype(BF16)
            return carry
        lax.fori_loop(0, cap // sub, back, 0)

    vspec = pl.BlockSpec(memory_space=pltpu.VMEM)
    return pl.pallas_call(
        kernel,
        in_specs=[vspec, vspec],
        out_specs=[vspec] * 6,
        out_shape=[jax.ShapeDtypeStruct((group_size, per), jnp.int32),
                   jax.ShapeDtypeStruct((1, cap), jnp.int32),
                   jax.ShapeDtypeStruct((1, slots), jnp.int32),
                   jax.ShapeDtypeStruct((8, pairs), jnp.int32),
                   jax.ShapeDtypeStruct((group_size, cap2), jnp.int32),
                   jax.ShapeDtypeStruct((cap, dim), BF16)],
        scratch_shapes=[pltpu.VMEM((rows_loc, 8, LANES), F32), pltpu.VMEM((cap, 8, LANES), F32),
                        pltpu.SMEM((1, cap), jnp.int32), pltpu.SemaphoreType.DMA(())],
        compiler_params=pltpu.CompilerParams(vmem_limit_bytes=VMEM_MAX),
        name="pack_rows",
    )(ids_h, table_loc)


def flat(ref):
    return ref.reshape(ref.shape[0] * 8, LANES)


def to_rows(dst, base, xf):
    r = xf.shape[0]
    for k in range(8):
        flat(dst)[pl.ds(base * 8 + k, r, stride=8), :] = xf[:, k * LANES:(k + 1) * LANES]


def from_rows(src, base, r):
    return jnp.concatenate([flat(src)[pl.ds(base * 8 + k, r, stride=8), :] for k in range(8)], axis=1)


def gather_rows(dst, src, index, count, unroll=16):
    def body(i, c):
        for j in range(unroll):
            r = i * unroll + j
            dst[r] = src[index(r)]
        return c
    lax.fori_loop(0, count // unroll, body, 0)


def group_call(p_own, gidx, inv2, gain, w_loc, du4, dres, cap, cap2):
    n_micro, group_size, seq_loc, cols = du4.shape
    chips = group_size // 2
    dim = w_loc.shape[0]
    per = n_micro * seq_loc
    half = per // 2
    piece = half // 2
    hcap = cap // 2
    slots = group_size * cap2
    sub = 64
    far = chips // 2

    def kernel(gidx_ref, inv_ref, p_ref, g_ref, w_ref, du_ref, r_ref,
               pall_ref, n_ref, x_ref, pack_ref, dg_ref, dw_out,
               rows, land, stage, nbuf, ntr, dub, dw_ref, part, relay_in, relay_p, relay_out,
               own_p, direct, summed, dg_all, land_sem, du_sem, n_sem, send, recv):
        me = lax.axis_index('tp')
        c = me // 2
        k = me % 2

        def dev(chip_off, core):
            return ((c + chip_off) % chips) * 2 + core

        right, left, partner = dev(1, k), dev(chips - 1, k), dev(0, 1 - k)
        barrier = pltpu.get_barrier_semaphore()
        for o in range(1, group_size):
            pl.semaphore_signal(barrier, inc=1, device_id={'tp': (me + o) % group_size}, device_id_type=pl.DeviceIdType.MESH)
        pl.semaphore_wait(barrier, group_size - 1)

        def rcopy(src, dst, s, r, to):
            return pltpu.make_async_remote_copy(src_ref=src, dst_ref=dst, send_sem=send.at[s], recv_sem=recv.at[r],
                                                device_id={'tp': to}, device_id_type=pl.DeviceIdType.MESH)

        def arrived(dst, r):
            pltpu.make_async_remote_copy(src_ref=dst, dst_ref=dst, send_sem=send.at[0], recv_sem=recv.at[r],
                                         device_id={'tp': partner}, device_id_type=pl.DeviceIdType.MESH).wait_recv()

        sent = []

        def go(cp):
            cp.start()
            sent.append(cp)

        def blk(d, off=0, n=cap):
            return pall_ref.at[pl.ds(pl.multiple_of(d * cap + off, 16), n), :]

        def ph(i):
            return p_ref.at[pl.ds(i * hcap, hcap), :]

        go(rcopy(ph(0), blk(me, 0, hcap), 0, 0, right))
        go(rcopy(ph(1), blk(me, hcap, hcap), 1, 1, left))
        go(rcopy(p_ref, blk(me), 2, 2, partner))
        go(rcopy(ph(1), blk(me, hcap, hcap), 31, 31, right))
        go(rcopy(ph(0), blk(me, 0, hcap), 32, 32, left))

        def du_copy(d, slot):
            return pltpu.make_async_copy(du_ref.at[:, d], dub.at[slot], du_sem.at[slot])

        def order(j):
            return ((c + far + j // 2) % chips) * 2 + j % 2

        du_copy(order(0), 0).start()

        def dn_body(j, carry):
            slot = j % 2

            @pl.when(j + 1 < group_size)
            def _():
                du_copy(order(j + 1), 1 - slot).start()
            du_copy(order(j), slot).wait()
            d = order(j)
            dv = dub[slot].reshape(per, cols)
            for t in range(0, dim, 256):
                part[d, :, t:t + 256] = lax.dot_general(
                    dv, w_ref[t:t + 256, :], (((1,), (1,)), ((), ())), preferred_element_type=F32).astype(BF16)
            return carry
        lax.fori_loop(0, group_size, dn_body, 0)

        du_copy(0, 0).start()

        def first_hop(kk):
            d = dev(far, kk)
            go(rcopy(part.at[d, pl.ds(0, half)], relay_in.at[0, k], 9 + kk, 9 + k, dev(chips - 1, kk)))
            go(rcopy(part.at[d, pl.ds(half, half)], relay_in.at[1, k], 11 + kk, 11 + k, dev(1, kk)))

        arrived(blk(left, 0, hcap), 0)
        go(rcopy(blk(left, 0, hcap), blk(left, 0, hcap), 3, 3, right))
        arrived(blk(right, hcap, hcap), 1)
        go(rcopy(blk(right, hcap, hcap), blk(right, hcap, hcap), 4, 4, left))
        first_hop(0)
        first_hop(1)
        for kk in range(2):
            go(rcopy(part.at[dev(chips - 1, kk), pl.ds(half, half)], direct.at[1, k], 13 + kk, 13 + k, dev(chips - 1, kk)))
            go(rcopy(part.at[dev(1, kk), pl.ds(0, half)], direct.at[0, k], 15 + kk, 15 + k, dev(1, kk)))
        dl, dr = dev(chips - 1, 1 - k), dev(1, 1 - k)
        go(rcopy(part.at[dl, pl.ds(0, half)], relay_p.at[0], 17, 17, partner))
        go(rcopy(part.at[dr, pl.ds(half, half)], relay_p.at[1], 18, 18, partner))
        go(rcopy(part.at[partner], own_p, 19, 19, partner))

        def convert(src, base, n):
            cp = pltpu.make_async_copy(src, land.at[pl.ds(0, n), :], land_sem)
            cp.start()
            cp.wait()

            def body(i, carry):
                off = pl.multiple_of(i * sub, sub)
                to_rows(rows, base + off, land[pl.ds(off, sub), :].astype(F32))
                return carry
            lax.fori_loop(0, n // sub, body, 0)

        convert(p_ref, me * cap, cap)
        arrived(blk(partner), 2)
        convert(blk(partner), partner * cap, cap)

        arrived(blk(left, hcap, hcap), 31)
        go(rcopy(blk(left), blk(left), 5, 5, partner))
        arrived(blk(right, 0, hcap), 32)
        go(rcopy(blk(right), blk(right), 6, 6, partner))
        convert(blk(left), left * cap, cap)
        convert(blk(right), right * cap, cap)
        pl_, pr_ = dev(chips - 1, 1 - k), dev(1, 1 - k)
        arrived(blk(pl_), 5)
        convert(blk(pl_), pl_ * cap, cap)
        arrived(blk(pr_), 6)
        convert(blk(pr_), pr_ * cap, cap)
        fk, fp = dev(far, k), dev(far, 1 - k)
        arrived(blk(fk, 0, hcap), 3)
        go(rcopy(blk(fk, 0, hcap), blk(fk, 0, hcap), 7, 7, partner))
        convert(blk(fk, 0, hcap), fk * cap, hcap)
        arrived(blk(fk, hcap, hcap), 4)
        go(rcopy(blk(fk, hcap, hcap), blk(fk, hcap, hcap), 8, 8, partner))
        convert(blk(fk, hcap, hcap), fk * cap + hcap, hcap)
        arrived(blk(fp, 0, hcap), 7)
        convert(blk(fp, 0, hcap), fp * cap, hcap)
        arrived(blk(fp, hcap, hcap), 8)
        convert(blk(fp, hcap, hcap), fp * cap + hcap, hcap)

        relays = [[rcopy(relay_out.at[s, pl.ds(q * piece, piece)], summed.at[s, pl.ds(q * piece, piece)],
                         20 + 2 * s + q, 20 + 2 * s + q, left if s == 0 else right) for q in range(2)] for s in range(2)]

        def relay():
            for s in range(2):
                d = left if s == 0 else right
                arrived(relay_p.at[s], 17 + s)
                for kk in range(2):
                    arrived(relay_in.at[s, kk], 9 + 2 * s + kk)
                for q in range(2):
                    def body(i, carry):
                        o = pl.multiple_of(q * piece + i * sub, sub)
                        a = part[d, pl.ds(pl.multiple_of(s * half + o, sub), sub), :].astype(F32)
                        a = a + relay_p[s, pl.ds(o, sub), :].astype(F32)
                        a = a + relay_in[s, 0, pl.ds(o, sub), :].astype(F32)
                        a = a + relay_in[s, 1, pl.ds(o, sub), :].astype(F32)
                        relay_out[s, pl.ds(o, sub), :] = a
                        return carry
                    lax.fori_loop(0, piece // sub, body, 0)
            for q in range(2):
                for s in range(2):
                    relays[s][q].start()

        gf = g_ref[...].astype(F32)

        def n_copy(h, slot):
            return pltpu.make_async_copy(nbuf.at[slot], n_ref.at[:, h], n_sem.at[slot])

        def chunk(h, carry):
            slot = h % 2

            @pl.when(h == 3)
            def _():
                relay()

            @pl.when(h + 1 < group_size)
            def _():
                du_copy(h + 1, 1 - slot).start()
            gather_rows(stage, rows, lambda r: gidx_ref[h, r], per)

            @pl.when(h >= 2)
            def _():
                n_copy(h - 2, slot).wait()

            def norm(i, carry2):
                off = pl.multiple_of(i * sub, sub)
                ms = sub // seq_loc
                xf = from_rows(stage, off, sub)
                rs = lax.rsqrt(jnp.mean(xf * xf, axis=-1, keepdims=True) + NORM_EPS)
                nb = ((xf * rs) * gf).astype(BF16)
                nbuf[slot, pl.ds(i * ms, ms)] = nb.reshape(ms, seq_loc, dim)

                @pl.when(h == me)
                def _():
                    x_ref[pl.ds(i * ms, ms)] = xf.astype(BF16).reshape(ms, seq_loc, dim)
                return carry2
            lax.fori_loop(0, per // sub, norm, 0)
            n_copy(h, slot).start()
            ntr[...] = nbuf[slot].reshape(per, dim).T
            du_copy(h, slot).wait()
            for t in range(0, cols, 256):
                w = min(256, cols - t)
                dv = dub[slot, :, :, t:t + w].reshape(per, w)
                contrib = jnp.dot(ntr[...], dv, preferred_element_type=F32)

                @pl.when(h == 0)
                def _():
                    dw_ref[:, t:t + w] = contrib

                @pl.when(h > 0)
                def _():
                    dw_ref[:, t:t + w] += contrib
            return carry
        lax.fori_loop(0, group_size, chunk, 0)
        dw_copy = pltpu.make_async_copy(dw_ref, dw_out, land_sem)
        dw_copy.start()
        n_copy(group_size - 2, 0).wait()
        n_copy(group_size - 1, 1).wait()

        arrived(own_p, 19)
        for kk in range(2):
            arrived(direct.at[0, kk], 15 + kk)
            arrived(direct.at[1, kk], 13 + kk)
        for q in range(2):
            for s in range(2):
                arrived(summed.at[s, pl.ds(q * piece, piece)], 20 + 2 * s + q)

                def body(i, acc):
                    ms = sub // seq_loc
                    o = pl.multiple_of(q * piece + i * sub, sub)
                    f = pl.multiple_of(s * half + o, sub)
                    dn = summed[s, pl.ds(o, sub), :] + part[me, pl.ds(f, sub), :].astype(F32)
                    dn = dn + own_p[pl.ds(f, sub), :].astype(F32)
                    dn = dn + direct[s, 0, pl.ds(o, sub), :].astype(F32)
                    dn = dn + direct[s, 1, pl.ds(o, sub), :].astype(F32)
                    m0 = f // seq_loc
                    xf = x_ref[pl.ds(m0, ms)].reshape(sub, dim).astype(F32)
                    rs = lax.rsqrt(jnp.mean(xf * xf, axis=-1, keepdims=True) + NORM_EPS)
                    nh = xf * rs
                    gdn = gf * dn
                    centre = jnp.mean(nh * gdn, axis=-1, keepdims=True)
                    dres_f = r_ref[pl.ds(m0, ms)].reshape(sub, dim).astype(F32)
                    dx = (dres_f + rs * (gdn - nh * centre)).astype(BF16)
                    to_rows(stage, f, dx.astype(F32))
                    return acc + jnp.sum(dn * nh, axis=0, keepdims=True)
                got = lax.fori_loop(0, piece // sub, body, jnp.zeros((1, dim), F32))
                if q == 0 and s == 0:
                    dg_all[me] = got
                else:
                    dg_all[me] += got

        for o in range(1, group_size):
            go(rcopy(dg_all.at[me], dg_all.at[me], 23 + o, 23 + o, (me + o) % group_size))
        gather_rows(rows, stage, lambda r: inv_ref[0, r], slots)

        def out(i, carry):
            off = pl.multiple_of(i * sub, sub)
            pack_ref[pl.ds(off, sub), :] = from_rows(rows, off, sub).astype(BF16)
            return carry
        lax.fori_loop(0, slots // sub, out, 0)
        for o in range(1, group_size):
            arrived(dg_all.at[(me + group_size - o) % group_size], 23 + o)
        dg = dg_all[0]
        for o in range(1, group_size):
            dg = dg + dg_all[o]
        dg_ref[...] = dg
        dw_copy.wait()
        for cp in sent:
            cp.wait_send()
        for s in range(2):
            for q in range(2):
                relays[s][q].wait_send()

    anyspec = pl.BlockSpec(memory_space=pl.ANY)
    vspec = pl.BlockSpec(memory_space=pltpu.VMEM)
    sspec = pl.BlockSpec(memory_space=pltpu.SMEM)
    return pl.pallas_call(
        kernel,
        in_specs=[sspec, sspec, anyspec, vspec, vspec, anyspec, vspec],
        out_specs=[anyspec, anyspec, vspec, vspec, vspec, anyspec],
        out_shape=[jax.ShapeDtypeStruct((group_size * cap, dim), BF16),
                   jax.ShapeDtypeStruct((n_micro, group_size, seq_loc, dim), BF16),
                   jax.ShapeDtypeStruct((n_micro, seq_loc, dim), BF16),
                   jax.ShapeDtypeStruct((slots, dim), BF16),
                   jax.ShapeDtypeStruct((1, dim), F32),
                   jax.ShapeDtypeStruct((dim, cols), F32)],
        scratch_shapes=[pltpu.VMEM((group_size * cap, 8, LANES), F32),
                        pltpu.VMEM((cap, dim), BF16),
                        pltpu.VMEM((per, 8, LANES), F32),
                        pltpu.VMEM((2, n_micro, seq_loc, dim), BF16),
                        pltpu.VMEM((dim, per), BF16),
                        pltpu.VMEM((2, n_micro, seq_loc, cols), BF16),
                        pltpu.VMEM((dim, cols), F32),
                        pltpu.VMEM((group_size, per, dim), BF16),
                        pltpu.VMEM((2, 2, half, dim), BF16),
                        pltpu.VMEM((2, half, dim), BF16),
                        pltpu.VMEM((2, half, dim), F32),
                        pltpu.VMEM((per, dim), BF16),
                        pltpu.VMEM((2, 2, half, dim), BF16),
                        pltpu.VMEM((2, half, dim), F32),
                        pltpu.VMEM((group_size, 1, dim), F32),
                        pltpu.SemaphoreType.DMA(()),
                        pltpu.SemaphoreType.DMA((2,)),
                        pltpu.SemaphoreType.DMA((2,)),
                        pltpu.SemaphoreType.DMA((33,)),
                        pltpu.SemaphoreType.DMA((33,))],
        compiler_params=pltpu.CompilerParams(collective_id=0, has_side_effects=True, vmem_limit_bytes=66_900_000),
        name="group_rows",
    )(gidx, inv2, p_own, gain.reshape(1, dim), w_loc, du4, dres)


def table_grad_call(recv, tgt, dw, x, rows_loc):
    slots, dim = recv.shape
    group_size, cap2 = tgt.shape
    sub = 64
    steps = 8
    blk = rows_loc // steps
    unroll = 16

    def kernel(tgt_ref, r_ref, dw_in, x_in, o_ref, dw_out, x_out, land, rows, acc, out, dw_v, x_v, sem_r, sem_o, sem_w, sem_x):
        def local(a, b, s):
            return pltpu.make_async_copy(a, b, s)

        first = local(r_ref, land, sem_r)
        first.start()
        dw1, dw2 = local(dw_in, dw_v, sem_w), local(dw_v, dw_out, sem_w)
        x1, x2 = local(x_in, x_v, sem_x), local(x_v, x_out, sem_x)
        dw1.start()
        x1.start()

        def zero(i, carry):
            acc[pl.ds(i * sub, sub)] = jnp.zeros((sub, 8, LANES), F32)
            return carry
        lax.fori_loop(0, rows_loc // sub, zero, 0)
        first.wait()

        def conv(i, carry):
            off = pl.multiple_of(i * sub, sub)
            to_rows(rows, off, land[pl.ds(off, sub), :].astype(F32))
            return carry
        lax.fori_loop(0, slots // sub, conv, 0)
        dw1.wait()
        dw2.start()
        x1.wait()
        x2.start()
        for h in range(group_size):
            def add(i, carry):
                for j in range(unroll):
                    r = i * unroll + j
                    t = tgt_ref[h, r]
                    acc[t] = acc[t] + rows[h * cap2 + r]
                return carry
            lax.fori_loop(0, cap2 // unroll, add, 0)

        def put(c):
            return local(out.at[c % 2], o_ref.at[pl.ds(c * blk, blk), :], sem_o.at[c % 2])

        for c in range(steps):
            if c >= 2:
                put(c - 2).wait()

            def body(i, carry):
                off = pl.multiple_of(i * sub, sub)
                out[c % 2, pl.ds(off, sub), :] = from_rows(acc, c * blk + off, sub)
                return carry
            lax.fori_loop(0, blk // sub, body, 0)
            put(c).start()
        put(steps - 2).wait()
        put(steps - 1).wait()
        dw2.wait()
        x2.wait()

    anyspec = pl.BlockSpec(memory_space=pl.ANY)
    return pl.pallas_call(
        kernel,
        in_specs=[pl.BlockSpec(memory_space=pltpu.SMEM), anyspec, anyspec, anyspec],
        out_specs=[anyspec] * 3,
        out_shape=[jax.ShapeDtypeStruct((rows_loc, dim), F32), jax.ShapeDtypeStruct(dw.shape, dw.dtype), jax.ShapeDtypeStruct(x.shape, x.dtype)],
        scratch_shapes=[pltpu.VMEM((slots, dim), BF16), pltpu.VMEM((slots, 8, LANES), F32), pltpu.VMEM((rows_loc + 8, 8, LANES), F32),
                        pltpu.VMEM((2, blk, dim), F32), pltpu.VMEM(dw.shape, dw.dtype), pltpu.VMEM(x.shape, x.dtype),
                        pltpu.SemaphoreType.DMA(()), pltpu.SemaphoreType.DMA((2,)), pltpu.SemaphoreType.DMA(()), pltpu.SemaphoreType.DMA(())],
        compiler_params=pltpu.CompilerParams(vmem_limit_bytes=VMEM_MAX),
        cost_estimate=pl.CostEstimate(flops=2_000_000_000, bytes_accessed=24_000_000, transcendentals=0),
        name="table_grad",
    )(tgt, recv, dw, x)


def fast_step(tables, table_loc, gain_vec, w_loc, du_loc, dres_loc, group_size, cap, cap2):
    gidx, _, inv2, _, tgt, mine = tables
    n_micro, seq_len, cols = du_loc.shape
    seq_loc = seq_len // group_size
    rows_loc, dim = table_loc.shape
    du4 = du_loc.reshape(n_micro, group_size, seq_loc, cols)
    _, normed, x_own, dx_pack, dg, grad_w = group_call(mine, gidx, inv2, gain_vec, w_loc, du4, dres_loc, cap, cap2)
    nt = normed.reshape(n_micro * seq_len, dim)
    u = jnp.dot(nt, w_loc, preferred_element_type=F32).astype(BF16)
    recv = lax.all_to_all(dx_pack.reshape(group_size, cap2, dim), 'tp', 0, 0, tiled=True)
    grad_table, grad_w, x_own = table_grad_call(recv.reshape(group_size * cap2, dim), tgt, grad_w, x_own, rows_loc)
    grad_gain = dg.reshape(dim)
    return u.reshape(n_micro, seq_len, cols), x_own, grad_table, grad_w, grad_gain


def solution(mesh):
    group_size = mesh.shape['tp']

    def local_step(token_ids, table_loc, gain_vec, w_loc, du_loc, dres_loc):
        rows_loc = table_loc.shape[0]
        tokens = token_ids.shape[0] * token_ids.shape[1]
        cap = tokens // group_size * 5 // 4
        cap2 = tokens // group_size // group_size * 7 // 4
        tables = pack_call(token_ids, table_loc, group_size, cap, cap2)
        ok = (tables[3][2, 0] <= cap) & (tables[3][3, 0] <= cap2)
        return lax.cond(
            ok,
            lambda t, i, *a: fast_step(t, *a, group_size, cap, cap2),
            lambda t, i, *a: slow_step(i, *a, group_size),
            tuple(tables), token_ids, table_loc, gain_vec, w_loc, du_loc, dres_loc)

    return jax.shard_map(local_step, mesh=mesh,
                         in_specs=(P('dp', None), P('tp', None), P(None), P(None, 'tp'), P('dp', None, 'tp'), P('dp', 'tp', None)),
                         out_specs=(P('dp', None, 'tp'), P('dp', 'tp', None), P(('dp', 'tp'), None), P(None, ('dp', 'tp')), P('dp')),
                         check_vma=False)
```

```python
import functools
import jax
import jax.numpy as jnp
from jax import lax
from jax.experimental import pallas as pl
from jax.experimental.pallas import tpu as pltpu
from jax.sharding import PartitionSpec as P

NORM_EPS = 1e-6
LANES = 128
F32 = jnp.float32
BF16 = jnp.bfloat16
VMEM_MAX = 60 * 1024 * 1024


def _capacity(mean, slack):
    return -(-(mean * slack) // 128) * 128 // 8


def slow_step(token_ids, table_loc, gain_vec, w_loc, du_loc, dres_loc, group_size):
    seq_len = token_ids.shape[1]
    rows_loc, model_dim = table_loc.shape
    seq_loc = seq_len // group_size
    cols_loc = w_loc.shape[1]
    dev_idx = lax.axis_index('tp')
    row_start = dev_idx * rows_loc
    tok_start = dev_idx * seq_loc
    gain_f = gain_vec.astype(F32)

    def micro_step(acc_state, inputs):
        grad_table, grad_w, grad_gain = acc_state
        tok_ids, du_m, dres_m = inputs
        local_ids = tok_ids - row_start
        in_block = (local_ids >= 0) & (local_ids < rows_loc)
        safe_ids = jnp.where(in_block, local_ids, 0)
        looked = jnp.take(table_loc, safe_ids, axis=0)
        partial_x = jnp.where(in_block[:, None], looked, jnp.zeros_like(looked))
        spread = lax.all_to_all(partial_x.reshape(group_size, seq_loc, model_dim), 'tp', 0, 0, tiled=True)
        mine = jnp.sum(spread, axis=0, dtype=F32).astype(BF16)
        tokens = lax.all_gather(mine, 'tp', axis=0, tiled=True)
        tok_f = tokens.astype(F32)
        inv_rms = lax.rsqrt(jnp.mean(tok_f * tok_f, axis=-1, keepdims=True) + NORM_EPS)
        n_hat = tok_f * inv_rms
        normed = (n_hat * gain_f).astype(BF16)
        u_m = jnp.dot(normed, w_loc, preferred_element_type=F32).astype(BF16)
        x_own = lax.dynamic_slice_in_dim(tokens, tok_start, seq_loc, axis=0)
        dn_part = lax.dot_general(du_m, w_loc, (((1,), (1,)), ((), ())), preferred_element_type=F32).astype(BF16)
        dn_recv = lax.all_to_all(dn_part.reshape(group_size, seq_loc, model_dim), 'tp', 0, 0, tiled=True)
        d_norm = jnp.sum(dn_recv, axis=0, dtype=F32)
        hat_own = lax.dynamic_slice_in_dim(n_hat, tok_start, seq_loc, axis=0)
        inv_own = lax.dynamic_slice_in_dim(inv_rms, tok_start, seq_loc, axis=0)
        gain_dn = gain_f * d_norm
        centre = jnp.mean(hat_own * gain_dn, axis=-1, keepdims=True)
        d_x = (dres_m.astype(F32) + inv_own * (gain_dn - hat_own * centre)).astype(BF16)
        grad_gain = grad_gain + jnp.sum(d_norm * hat_own, axis=0)
        grad_w = grad_w + lax.dot_general(normed, du_m, (((0,), (0,)), ((), ())), preferred_element_type=F32)
        dx_all = lax.all_gather(d_x, 'tp', axis=0, tiled=True)
        contrib = jnp.where(in_block[:, None], dx_all.astype(F32), 0.0)
        grad_table = grad_table + jax.ops.segment_sum(contrib, safe_ids, num_segments=rows_loc)
        return (grad_table, grad_w, grad_gain), (u_m, x_own)

    init_state = (jnp.zeros((rows_loc, model_dim), F32), jnp.zeros((model_dim, cols_loc), F32), jnp.zeros((model_dim,), F32))
    (grad_table, grad_w, grad_gain), (u_proj, x_resid) = lax.scan(micro_step, init_state, (token_ids, du_loc, dres_loc))
    grad_gain = lax.psum(grad_gain, 'tp')
    return u_proj, x_resid, grad_table, grad_w, grad_gain


def pack_call(token_ids, table_loc, group_size, cap, cap2):
    n_micro, seq_len = token_ids.shape
    seq_loc = seq_len // group_size
    per = n_micro * seq_loc
    rows_loc, dim = table_loc.shape
    slots = group_size * cap2
    pairs = group_size * group_size
    sub = 64
    ids_h = token_ids.reshape(n_micro, group_size, seq_loc).transpose(1, 0, 2).reshape(group_size, per)

    def kernel(ids_ref, e_ref, gidx_ref, pid_ref, inv_ref, stat_ref, tgt_ref, p_ref, rows, stage, pid_s, sem):
        me = lax.axis_index('tp')
        ids = ids_ref[...]
        owner = ids // rows_loc
        oh = jnp.concatenate([(owner == o).astype(F32) for o in range(group_size)], axis=0)
        ohb = oh.astype(BF16)
        tri = (lax.broadcasted_iota(jnp.int32, (per, per), 0) < lax.broadcasted_iota(jnp.int32, (per, per), 1)).astype(F32).astype(BF16)
        rank = jnp.dot(ohb, tri, preferred_element_type=F32)
        nt = (((1,), (1,)), ((), ()))
        cnt_row = lax.dot_general(jnp.ones((8, per), BF16), ohb, nt, preferred_element_type=F32)[0:1]
        cnt_col = jnp.sum(oh, axis=1, keepdims=True)
        ra = lax.broadcasted_iota(jnp.int32, (pairs, pairs), 0)
        rb = lax.broadcasted_iota(jnp.int32, (pairs, pairs), 1)
        same = ra // group_size == rb // group_size
        base_col = jnp.sum(jnp.where(same & (rb < ra), cnt_row, 0.0), axis=1, keepdims=True)
        base_row = jnp.sum(jnp.where(same & (ra < rb), cnt_col, 0.0), axis=0, keepdims=True)
        tot_row = jnp.sum(jnp.where(same, cnt_col, 0.0), axis=0, keepdims=True)
        worst = jnp.concatenate([jnp.max(tot_row, axis=1, keepdims=True), jnp.max(cnt_row, axis=1, keepdims=True)], axis=0)

        def fold(v):
            s = v[0:group_size]
            for o in range(1, group_size):
                s = s + v[o * group_size:(o + 1) * group_size]
            return s.astype(jnp.int32)

        rk = fold(oh * rank)
        grank = fold(oh * (rank + base_col))
        gidx_ref[...] = owner * cap + jnp.minimum(grank, cap - 1)
        stat_ref[0:1, :] = cnt_row.astype(jnp.int32)
        stat_ref[1:2, :] = base_row.astype(jnp.int32)
        stat_ref[2:4, :] = jnp.broadcast_to(worst, (2, pairs)).astype(jnp.int32)
        stat_ref[4:8, :] = jnp.zeros((4, pairs), jnp.int32)

        def place(slot, value, n):
            hot = (slot == lax.broadcasted_iota(jnp.int32, (n, per), 0)).astype(F32).astype(BF16)
            parts = jnp.concatenate([value // 64, value % 64] + [jnp.zeros_like(value)] * 6, axis=0).astype(F32).astype(BF16)
            return lax.dot_general(parts, hot, nt, preferred_element_type=F32)

        mine = jnp.where(owner == me, grank, -1)
        local = jnp.clip(ids - me * rows_loc, 0, rows_loc - 1)
        acc = jnp.zeros((8, cap), F32)
        for h in range(group_size):
            acc = acc + place(mine[h:h + 1], local[h:h + 1], cap)
        pid = (acc[0:1] * 64.0 + acc[1:2]).astype(jnp.int32)
        pid_ref[...] = pid
        pair = jnp.where(owner == me, rk, -1)
        for h in range(group_size):
            got = place(pair[h:h + 1], local[h:h + 1] + 1, cap2)
            row = (got[0:1] * 64.0 + got[1:2]).astype(jnp.int32)
            tgt_ref[h:h + 1, :] = jnp.where(row == 0, rows_loc, row - 1)
        own = lax.broadcasted_iota(jnp.int32, (group_size, 1), 0) == me
        slot2 = jnp.sum(jnp.where(own, owner * cap2 + rk, 0), axis=0, keepdims=True)
        put = place(slot2, lax.broadcasted_iota(jnp.int32, (1, per), 1), slots)
        inv_ref[...] = (put[0:1] * 64.0 + put[1:2]).astype(jnp.int32)
        cp = pltpu.make_async_copy(pid_ref, pid_s, sem)
        cp.start()

        def conv(i, carry):
            off = pl.multiple_of(i * sub, sub)
            to_rows(rows, off, e_ref[pl.ds(off, sub), :].astype(F32))
            return carry
        lax.fori_loop(0, rows_loc // sub, conv, 0)
        cp.wait()
        gather_rows(stage, rows, lambda r: pid_s[0, r], cap)

        def back(i, carry):
            off = pl.multiple_of(i * sub, sub)
            p_ref[pl.ds(off, sub), :] = from_rows(stage, off, sub).astype(BF16)
            return carry
        lax.fori_loop(0, cap // sub, back, 0)

    vspec = pl.BlockSpec(memory_space=pltpu.VMEM)
    return pl.pallas_call(
        kernel,
        in_specs=[vspec, vspec],
        out_specs=[vspec] * 6,
        out_shape=[jax.ShapeDtypeStruct((group_size, per), jnp.int32),
                   jax.ShapeDtypeStruct((1, cap), jnp.int32),
                   jax.ShapeDtypeStruct((1, slots), jnp.int32),
                   jax.ShapeDtypeStruct((8, pairs), jnp.int32),
                   jax.ShapeDtypeStruct((group_size, cap2), jnp.int32),
                   jax.ShapeDtypeStruct((cap, dim), BF16)],
        scratch_shapes=[pltpu.VMEM((rows_loc, 8, LANES), F32), pltpu.VMEM((cap, 8, LANES), F32),
                        pltpu.SMEM((1, cap), jnp.int32), pltpu.SemaphoreType.DMA(())],
        compiler_params=pltpu.CompilerParams(vmem_limit_bytes=VMEM_MAX),
        name="pack_rows",
    )(ids_h, table_loc)


def flat(ref):
    return ref.reshape(ref.shape[0] * 8, LANES)


def to_rows(dst, base, xf):
    r = xf.shape[0]
    for k in range(8):
        flat(dst)[pl.ds(base * 8 + k, r, stride=8), :] = xf[:, k * LANES:(k + 1) * LANES]


def from_rows(src, base, r):
    return jnp.concatenate([flat(src)[pl.ds(base * 8 + k, r, stride=8), :] for k in range(8)], axis=1)


def gather_rows(dst, src, index, count, unroll=16):
    def body(i, c):
        for j in range(unroll):
            r = i * unroll + j
            dst[r] = src[index(r)]
        return c
    lax.fori_loop(0, count // unroll, body, 0)


def group_call(p_own, gidx, inv2, gain, w_loc, du4, dres, cap, cap2):
    n_micro, group_size, seq_loc, cols = du4.shape
    chips = group_size // 2
    dim = w_loc.shape[0]
    per = n_micro * seq_loc
    half = per // 2
    piece = half // 2
    hcap = cap // 2
    slots = group_size * cap2
    sub = 64
    far = chips // 2

    def kernel(gidx_ref, inv_ref, p_ref, g_ref, w_ref, du_ref, r_ref,
               pall_ref, n_ref, x_ref, pack_ref, dg_ref, dw_out,
               rows, land, stage, nbuf, ntr, dub, dw_ref, part, relay_in, relay_p, relay_out,
               own_p, direct, summed, dg_all, land_sem, du_sem, n_sem, send, recv):
        me = lax.axis_index('tp')
        c = me // 2
        k = me % 2

        def dev(chip_off, core):
            return ((c + chip_off) % chips) * 2 + core

        right, left, partner = dev(1, k), dev(chips - 1, k), dev(0, 1 - k)
        barrier = pltpu.get_barrier_semaphore()
        for o in range(1, group_size):
            pl.semaphore_signal(barrier, inc=1, device_id={'tp': (me + o) % group_size}, device_id_type=pl.DeviceIdType.MESH)
        pl.semaphore_wait(barrier, group_size - 1)

        def rcopy(src, dst, s, r, to):
            return pltpu.make_async_remote_copy(src_ref=src, dst_ref=dst, send_sem=send.at[s], recv_sem=recv.at[r],
                                                device_id={'tp': to}, device_id_type=pl.DeviceIdType.MESH)

        def arrived(dst, r):
            pltpu.make_async_remote_copy(src_ref=dst, dst_ref=dst, send_sem=send.at[0], recv_sem=recv.at[r],
                                         device_id={'tp': partner}, device_id_type=pl.DeviceIdType.MESH).wait_recv()

        sent = []

        def go(cp):
            cp.start()
            sent.append(cp)

        def blk(d, off=0, n=cap):
            return pall_ref.at[pl.ds(pl.multiple_of(d * cap + off, 16), n), :]

        def ph(i):
            return p_ref.at[pl.ds(i * hcap, hcap), :]

        go(rcopy(ph(0), blk(me, 0, hcap), 0, 0, right))
        go(rcopy(ph(1), blk(me, hcap, hcap), 1, 1, left))
        go(rcopy(p_ref, blk(me), 2, 2, partner))
        go(rcopy(ph(1), blk(me, hcap, hcap), 31, 31, right))
        go(rcopy(ph(0), blk(me, 0, hcap), 32, 32, left))

        def du_copy(d, slot):
            return pltpu.make_async_copy(du_ref.at[:, d], dub.at[slot], du_sem.at[slot])

        def order(j):
            return ((c + far + j // 2) % chips) * 2 + j % 2

        du_copy(order(0), 0).start()

        def dn_body(j, carry):
            slot = j % 2

            @pl.when(j + 1 < group_size)
            def _():
                du_copy(order(j + 1), 1 - slot).start()
            du_copy(order(j), slot).wait()
            d = order(j)
            dv = dub[slot].reshape(per, cols)
            for t in range(0, dim, 256):
                part[d, :, t:t + 256] = lax.dot_general(
                    dv, w_ref[t:t + 256, :], (((1,), (1,)), ((), ())), preferred_element_type=F32).astype(BF16)
            return carry
        lax.fori_loop(0, group_size, dn_body, 0)

        du_copy(0, 0).start()

        def first_hop(kk):
            d = dev(far, kk)
            go(rcopy(part.at[d, pl.ds(0, half)], relay_in.at[0, k], 9 + kk, 9 + k, dev(chips - 1, kk)))
            go(rcopy(part.at[d, pl.ds(half, half)], relay_in.at[1, k], 11 + kk, 11 + k, dev(1, kk)))

        arrived(blk(left, 0, hcap), 0)
        go(rcopy(blk(left, 0, hcap), blk(left, 0, hcap), 3, 3, right))
        arrived(blk(right, hcap, hcap), 1)
        go(rcopy(blk(right, hcap, hcap), blk(right, hcap, hcap), 4, 4, left))
        first_hop(0)
        first_hop(1)
        for kk in range(2):
            go(rcopy(part.at[dev(chips - 1, kk), pl.ds(half, half)], direct.at[1, k], 13 + kk, 13 + k, dev(chips - 1, kk)))
            go(rcopy(part.at[dev(1, kk), pl.ds(0, half)], direct.at[0, k], 15 + kk, 15 + k, dev(1, kk)))
        dl, dr = dev(chips - 1, 1 - k), dev(1, 1 - k)
        go(rcopy(part.at[dl, pl.ds(0, half)], relay_p.at[0], 17, 17, partner))
        go(rcopy(part.at[dr, pl.ds(half, half)], relay_p.at[1], 18, 18, partner))
        go(rcopy(part.at[partner], own_p, 19, 19, partner))

        def convert(src, base, n):
            cp = pltpu.make_async_copy(src, land.at[pl.ds(0, n), :], land_sem)
            cp.start()
            cp.wait()

            def body(i, carry):
                off = pl.multiple_of(i * sub, sub)
                to_rows(rows, base + off, land[pl.ds(off, sub), :].astype(F32))
                return carry
            lax.fori_loop(0, n // sub, body, 0)

        convert(p_ref, me * cap, cap)
        arrived(blk(partner), 2)
        convert(blk(partner), partner * cap, cap)

        arrived(blk(left, hcap, hcap), 31)
        go(rcopy(blk(left), blk(left), 5, 5, partner))
        arrived(blk(right, 0, hcap), 32)
        go(rcopy(blk(right), blk(right), 6, 6, partner))
        convert(blk(left), left * cap, cap)
        convert(blk(right), right * cap, cap)
        pl_, pr_ = dev(chips - 1, 1 - k), dev(1, 1 - k)
        arrived(blk(pl_), 5)
        convert(blk(pl_), pl_ * cap, cap)
        arrived(blk(pr_), 6)
        convert(blk(pr_), pr_ * cap, cap)
        fk, fp = dev(far, k), dev(far, 1 - k)
        arrived(blk(fk, 0, hcap), 3)
        go(rcopy(blk(fk, 0, hcap), blk(fk, 0, hcap), 7, 7, partner))
        convert(blk(fk, 0, hcap), fk * cap, hcap)
        arrived(blk(fk, hcap, hcap), 4)
        go(rcopy(blk(fk, hcap, hcap), blk(fk, hcap, hcap), 8, 8, partner))
        convert(blk(fk, hcap, hcap), fk * cap + hcap, hcap)
        arrived(blk(fp, 0, hcap), 7)
        convert(blk(fp, 0, hcap), fp * cap, hcap)
        arrived(blk(fp, hcap, hcap), 8)
        convert(blk(fp, hcap, hcap), fp * cap + hcap, hcap)

        relays = [[rcopy(relay_out.at[s, pl.ds(q * piece, piece)], summed.at[s, pl.ds(q * piece, piece)],
                         20 + 2 * s + q, 20 + 2 * s + q, left if s == 0 else right) for q in range(2)] for s in range(2)]

        def relay():
            for s in range(2):
                d = left if s == 0 else right
                arrived(relay_p.at[s], 17 + s)
                for kk in range(2):
                    arrived(relay_in.at[s, kk], 9 + 2 * s + kk)
                for q in range(2):
                    def body(i, carry):
                        o = pl.multiple_of(q * piece + i * sub, sub)
                        a = part[d, pl.ds(pl.multiple_of(s * half + o, sub), sub), :].astype(F32)
                        a = a + relay_p[s, pl.ds(o, sub), :].astype(F32)
                        a = a + relay_in[s, 0, pl.ds(o, sub), :].astype(F32)
                        a = a + relay_in[s, 1, pl.ds(o, sub), :].astype(F32)
                        relay_out[s, pl.ds(o, sub), :] = a
                        return carry
                    lax.fori_loop(0, piece // sub, body, 0)
            for q in range(2):
                for s in range(2):
                    relays[s][q].start()

        gf = g_ref[...].astype(F32).reshape(1, dim)

        def n_copy(h, slot):
            return pltpu.make_async_copy(nbuf.at[slot], n_ref.at[:, h], n_sem.at[slot])

        def chunk(h, carry):
            slot = h % 2

            @pl.when(h == 3)
            def _():
                relay()

            @pl.when(h + 1 < group_size)
            def _():
                du_copy(h + 1, 1 - slot).start()
            gather_rows(stage, rows, lambda r: gidx_ref[h, r], per)

            @pl.when(h >= 2)
            def _():
                n_copy(h - 2, slot).wait()

            def norm(i, carry2):
                off = pl.multiple_of(i * sub, sub)
                ms = sub // seq_loc
                xf = from_rows(stage, off, sub)
                rs = lax.rsqrt(jnp.mean(xf * xf, axis=-1, keepdims=True) + NORM_EPS)
                nb = ((xf * rs) * gf).astype(BF16)
                nbuf[slot, pl.ds(i * ms, ms)] = nb.reshape(ms, seq_loc, dim)

                @pl.when(h == me)
                def _():
                    x_ref[pl.ds(i * ms, ms)] = xf.astype(BF16).reshape(ms, seq_loc, dim)
                return carry2
            lax.fori_loop(0, per // sub, norm, 0)
            n_copy(h, slot).start()
            ntr[...] = nbuf[slot].reshape(per, dim).T
            du_copy(h, slot).wait()
            for t in range(0, cols, 256):
                w = min(256, cols - t)
                dv = dub[slot, :, :, t:t + w].reshape(per, w)
                contrib = jnp.dot(ntr[...], dv, preferred_element_type=F32)

                @pl.when(h == 0)
                def _():
                    dw_ref[:, t:t + w] = contrib

                @pl.when(h > 0)
                def _():
                    dw_ref[:, t:t + w] += contrib
            return carry
        lax.fori_loop(0, group_size, chunk, 0)
        dw_copy = pltpu.make_async_copy(dw_ref, dw_out, land_sem)
        dw_copy.start()
        n_copy(group_size - 2, 0).wait()
        n_copy(group_size - 1, 1).wait()

        arrived(own_p, 19)
        for kk in range(2):
            arrived(direct.at[0, kk], 15 + kk)
            arrived(direct.at[1, kk], 13 + kk)
        for q in range(2):
            for s in range(2):
                arrived(summed.at[s, pl.ds(q * piece, piece)], 20 + 2 * s + q)

                def body(i, acc):
                    ms = sub // seq_loc
                    o = pl.multiple_of(q * piece + i * sub, sub)
                    f = pl.multiple_of(s * half + o, sub)
                    dn = summed[s, pl.ds(o, sub), :] + part[me, pl.ds(f, sub), :].astype(F32)
                    dn = dn + own_p[pl.ds(f, sub), :].astype(F32)
                    dn = dn + direct[s, 0, pl.ds(o, sub), :].astype(F32)
                    dn = dn + direct[s, 1, pl.ds(o, sub), :].astype(F32)
                    m0 = f // seq_loc
                    xf = x_ref[pl.ds(m0, ms)].reshape(sub, dim).astype(F32)
                    rs = lax.rsqrt(jnp.mean(xf * xf, axis=-1, keepdims=True) + NORM_EPS)
                    nh = xf * rs
                    gdn = gf * dn
                    centre = jnp.mean(nh * gdn, axis=-1, keepdims=True)
                    dres_f = r_ref[pl.ds(m0, ms)].reshape(sub, dim).astype(F32)
                    dx = (dres_f + rs * (gdn - nh * centre)).astype(BF16)
                    to_rows(stage, f, dx.astype(F32))
                    return acc + jnp.sum(dn * nh, axis=0, keepdims=True)
                got = lax.fori_loop(0, piece // sub, body, jnp.zeros((1, dim), F32))
                if q == 0 and s == 0:
                    dg_all[me] = got
                else:
                    dg_all[me] += got

        for o in range(1, group_size):
            go(rcopy(dg_all.at[me], dg_all.at[me], 23 + o, 23 + o, (me + o) % group_size))
        gather_rows(rows, stage, lambda r: inv_ref[0, r], slots)

        def out(i, carry):
            off = pl.multiple_of(i * sub, sub)
            pack_ref[pl.ds(off, sub), :] = from_rows(rows, off, sub).astype(BF16)
            return carry
        lax.fori_loop(0, slots // sub, out, 0)
        for o in range(1, group_size):
            arrived(dg_all.at[(me + group_size - o) % group_size], 23 + o)
        dg = dg_all[0]
        for o in range(1, group_size):
            dg = dg + dg_all[o]
        dg_ref[...] = dg
        dw_copy.wait()
        for cp in sent:
            cp.wait_send()
        for s in range(2):
            for q in range(2):
                relays[s][q].wait_send()

    anyspec = pl.BlockSpec(memory_space=pl.ANY)
    vspec = pl.BlockSpec(memory_space=pltpu.VMEM)
    sspec = pl.BlockSpec(memory_space=pltpu.SMEM)
    return pl.pallas_call(
        kernel,
        in_specs=[sspec, sspec, anyspec, vspec, vspec, anyspec, vspec],
        out_specs=[anyspec, anyspec, vspec, vspec, vspec, anyspec],
        out_shape=[jax.ShapeDtypeStruct((group_size * cap, dim), BF16),
                   jax.ShapeDtypeStruct((n_micro, group_size, seq_loc, dim), BF16),
                   jax.ShapeDtypeStruct((n_micro, seq_loc, dim), BF16),
                   jax.ShapeDtypeStruct((slots, dim), BF16),
                   jax.ShapeDtypeStruct((1, dim), F32),
                   jax.ShapeDtypeStruct((dim, cols), F32)],
        scratch_shapes=[pltpu.VMEM((group_size * cap, 8, LANES), F32),
                        pltpu.VMEM((cap, dim), BF16),
                        pltpu.VMEM((per, 8, LANES), F32),
                        pltpu.VMEM((2, n_micro, seq_loc, dim), BF16),
                        pltpu.VMEM((dim, per), BF16),
                        pltpu.VMEM((2, n_micro, seq_loc, cols), BF16),
                        pltpu.VMEM((dim, cols), F32),
                        pltpu.VMEM((group_size, per, dim), BF16),
                        pltpu.VMEM((2, 2, half, dim), BF16),
                        pltpu.VMEM((2, half, dim), BF16),
                        pltpu.VMEM((2, half, dim), F32),
                        pltpu.VMEM((per, dim), BF16),
                        pltpu.VMEM((2, 2, half, dim), BF16),
                        pltpu.VMEM((2, half, dim), F32),
                        pltpu.VMEM((group_size, 1, dim), F32),
                        pltpu.SemaphoreType.DMA(()),
                        pltpu.SemaphoreType.DMA((2,)),
                        pltpu.SemaphoreType.DMA((2,)),
                        pltpu.SemaphoreType.DMA((33,)),
                        pltpu.SemaphoreType.DMA((33,))],
        compiler_params=pltpu.CompilerParams(collective_id=0, has_side_effects=True, vmem_limit_bytes=66_900_000),
        name="group_rows",
    )(gidx, inv2, p_own, gain, w_loc, du4, dres)


def table_grad_call(recv, tgt, dw, x, rows_loc):
    slots, dim = recv.shape
    group_size, cap2 = tgt.shape
    sub = 64
    steps = 8
    blk = rows_loc // steps
    unroll = 16

    def kernel(tgt_ref, r_ref, dw_in, x_in, o_ref, dw_out, x_out, land, rows, acc, out, dw_v, x_v, sem_r, sem_o, sem_w, sem_x):
        def local(a, b, s):
            return pltpu.make_async_copy(a, b, s)

        first = local(r_ref, land, sem_r)
        first.start()
        dw1, dw2 = local(dw_in, dw_v, sem_w), local(dw_v, dw_out, sem_w)
        x1, x2 = local(x_in, x_v, sem_x), local(x_v, x_out, sem_x)
        dw1.start()
        x1.start()

        def zero(i, carry):
            acc[pl.ds(i * sub, sub)] = jnp.zeros((sub, 8, LANES), F32)
            return carry
        lax.fori_loop(0, rows_loc // sub, zero, 0)
        first.wait()

        def conv(i, carry):
            off = pl.multiple_of(i * sub, sub)
            to_rows(rows, off, land[pl.ds(off, sub), :].astype(F32))
            return carry
        lax.fori_loop(0, slots // sub, conv, 0)
        dw1.wait()
        dw2.start()
        x1.wait()
        x2.start()
        for h in range(group_size):
            def add(i, carry):
                for j in range(unroll):
                    r = i * unroll + j
                    t = tgt_ref[h, r]
                    acc[t] = acc[t] + rows[h * cap2 + r]
                return carry
            lax.fori_loop(0, cap2 // unroll, add, 0)

        def put(c):
            return local(out.at[c % 2], o_ref.at[pl.ds(c * blk, blk), :], sem_o.at[c % 2])

        for c in range(steps):
            if c >= 2:
                put(c - 2).wait()

            def body(i, carry):
                off = pl.multiple_of(i * sub, sub)
                out[c % 2, pl.ds(off, sub), :] = from_rows(acc, c * blk + off, sub)
                return carry
            lax.fori_loop(0, blk // sub, body, 0)
            put(c).start()
        put(steps - 2).wait()
        put(steps - 1).wait()
        dw2.wait()
        x2.wait()

    anyspec = pl.BlockSpec(memory_space=pl.ANY)
    return pl.pallas_call(
        kernel,
        in_specs=[pl.BlockSpec(memory_space=pltpu.SMEM), anyspec, anyspec, anyspec],
        out_specs=[anyspec] * 3,
        out_shape=[jax.ShapeDtypeStruct((rows_loc, dim), F32), jax.ShapeDtypeStruct(dw.shape, dw.dtype), jax.ShapeDtypeStruct(x.shape, x.dtype)],
        scratch_shapes=[pltpu.VMEM((slots, dim), BF16), pltpu.VMEM((slots, 8, LANES), F32), pltpu.VMEM((rows_loc + 8, 8, LANES), F32),
                        pltpu.VMEM((2, blk, dim), F32), pltpu.VMEM(dw.shape, dw.dtype), pltpu.VMEM(x.shape, x.dtype),
                        pltpu.SemaphoreType.DMA(()), pltpu.SemaphoreType.DMA((2,)), pltpu.SemaphoreType.DMA(()), pltpu.SemaphoreType.DMA(())],
        compiler_params=pltpu.CompilerParams(vmem_limit_bytes=VMEM_MAX),
        cost_estimate=pl.CostEstimate(flops=2_000_000_000, bytes_accessed=24_000_000, transcendentals=0),
        name="table_grad",
    )(tgt, recv, dw, x)


def exchange(normed, x_own, dx_pack, dg, grad_w, tgt, w_loc, rows_loc):
    n_micro, group_size, seq_loc, dim = normed.shape
    cap2 = tgt.shape[1]
    cols = w_loc.shape[1]
    u = jnp.dot(normed.reshape(-1, dim), w_loc, preferred_element_type=F32).astype(BF16)
    recv = lax.all_to_all(dx_pack.reshape(group_size, cap2, dim), 'tp', 0, 0, tiled=True)
    grad_table, grad_w, x_own = table_grad_call(recv.reshape(group_size * cap2, dim), tgt, grad_w, x_own, rows_loc)
    return u.reshape(n_micro, group_size * seq_loc, cols), x_own, grad_table, grad_w, dg.reshape(dim)


def solution(mesh):
    group_size = mesh.shape['tp']

    def local_step(token_ids, table_loc, gain_vec, w_loc, du_loc, dres_loc):
        rows_loc = table_loc.shape[0]
        tokens = token_ids.shape[0] * token_ids.shape[1]
        cap = tokens // group_size * 5 // 4
        cap2 = tokens // group_size // group_size * 7 // 4
        n_micro, seq_len, cols = du_loc.shape
        gidx, _, inv2, stat, tgt, mine = pack_call(token_ids, table_loc, group_size, cap, cap2)
        ok = (stat[2, 0] <= cap) & (stat[3, 0] <= cap2)
        du4 = du_loc.reshape(n_micro, group_size, seq_len // group_size, cols)
        _, *mid = group_call(mine, gidx, inv2, gain_vec, w_loc, du4, dres_loc, cap, cap2)
        return lax.cond(
            ok,
            lambda mid, tgt, i, t, g, w, *a: exchange(*mid, tgt, w, rows_loc),
            lambda mid, tgt, *a: slow_step(*a, group_size),
            tuple(mid), tgt, token_ids, table_loc, gain_vec, w_loc, du_loc, dres_loc)

    return jax.shard_map(local_step, mesh=mesh,
                         in_specs=(P('dp', None), P('tp', None), P(None), P(None, 'tp'), P('dp', None, 'tp'), P('dp', 'tp', None)),
                         out_specs=(P('dp', None, 'tp'), P('dp', 'tp', None), P(('dp', 'tp'), None), P(None, ('dp', 'tp')), P('dp')),
                         check_vma=False)
```
